32 devices in a mesh: head: 2 (over core), seq: 8 (over z, y), mp: 2 (over x).
Axes of the slice: x: 2, y: 2, z: 4, core: 2. Of those that a mesh axis runs over, the one named last changes fastest.
Arguments:
- trunk: bfloat16 [128, 8192], P('seq', 'mp'), may hold values from -6 to 6
- branch: bfloat16 [2, 128, 8192], P('head', 'seq', 'mp'), may hold values from -6 to 6
- unembed: bfloat16 [18432, 8192], P('seq', 'mp'), may hold values from -0.09375 to 0.09375
- targets: int32 [2, 128], P('head'), may hold values from 0 to 18431
- loss_grad: float32 [2, 128], P('head'), may hold values from 0.25 to 4
Outputs:
- d_branch: bfloat16 [2, 128, 8192], P('head', 'seq', 'mp')
- d_trunk: bfloat16 [128, 8192], P('seq', 'mp')
- d_unembed: float32 [18432, 8192], P('seq', 'mp')
The draws below stay inside these ranges and needn't reach their ends.
All inputs are finite; a program needn't handle non-finite values.
Results may differ from the reference program's by a relative error of at most 0.0051.
Values may be sent and summed in bfloat16 or wider, within the bound.
No kernel may reach another device: no remote copies, remote signals or barrier semaphores. Data moves between devices by JAX's collectives and lax.ppermute only.
A program may use at most 192 MiB of HBM per device.

```python
import math
import jax
import jax.numpy as jnp

D = 8192
V = 18432
TOKENS = 128
HEADS = 2


def plant(array, key, low, high):
    longest = array.shape.index(max(array.shape))
    spots = []
    for shift in (0, 1):
        where = [jax.random.randint(jax.random.fold_in(key, axis), (), 0, length) for axis, length in enumerate(array.shape)]
        where[longest] = (where[longest] + shift) % array.shape[longest]
        spots.append(tuple(where))
    return array.at[spots[0]].set(low).at[spots[1]].set(high)


def steps_of(key, extent, pieces, least, largest):
    def one(axis_at, parts):
        draws = jax.random.uniform(jax.random.fold_in(jax.random.fold_in(key, 6), axis_at), (parts,), jnp.float32, least / len(pieces), largest / len(pieces))
        return jnp.repeat(jnp.exp(draws), extent[axis_at] // parts).reshape((-1,) + (1,) * (len(extent) - axis_at - 1))

    gain = one(*pieces[0])
    for cut in pieces[1:]:
        gain = gain * one(*cut)
    return gain


def noise(own_key, shape, width, most, cuts=(), kind=jnp.bfloat16):
    values = jax.random.normal(own_key, shape, jnp.float32) * width
    if len(cuts) > 0:
        values = steps_of(own_key, shape, cuts, -0.22, 0.18) * values
    return jnp.clip(values, min=-most, max=most).astype(kind)


def setup_inputs(seed: int = 0) -> dict:
    key_of = jax.random.split(jax.random.key(seed), 6)
    return {
        "trunk": noise(key_of[0], (TOKENS, D), 1.0, 6.0, ((0, 8), (1, 2))),
        "branch": noise(key_of[1], (HEADS, TOKENS, D), 1.0, 6.0, ((0, 2), (1, 8), (2, 2))),
        "unembed": noise(key_of[2], (V, D), (D * 4 // 9) ** -0.5, 0.09375, ((0, 8), (1, 2))),
        "targets": plant(jax.random.randint(key_of[3], (HEADS, TOKENS), 0, V), jax.random.fold_in(key_of[3], 1), 0, V - 1).astype(jnp.int32),
        "loss_grad": jnp.clip(jnp.exp(math.log(4.0) - 2.7725887 * jax.random.uniform(key_of[4], (HEADS, TOKENS), jnp.float32) ** steps_of(key_of[4], (HEADS, TOKENS), ((0, 2),), -0.2, 0.2)), 0.25, 4.0),
    }


soft_cap = 30.0


def reference(trunk, branch, unembed, targets, loss_grad):
    vocab_ids = jnp.arange(V, dtype=jnp.int32)
    grads = []
    trunk_grad = jnp.zeros((TOKENS, D), jnp.float32)
    unembed_grad = jnp.zeros((V, D), jnp.float32)
    for which in range(HEADS):
        hidden = (trunk.astype(jnp.float32) + branch[which].astype(jnp.float32)).astype(jnp.bfloat16)
        scores = jnp.dot(hidden, unembed.T, preferred_element_type=jnp.float32)
        squashed = jnp.tanh(scores / soft_cap)
        exponent = jnp.exp(soft_cap * squashed)
        totals = jnp.sum(exponent, axis=1)
        onehot = (targets[which][:, None] == vocab_ids[None, :]).astype(jnp.float32)
        slope = loss_grad[which][:, None] * (exponent / totals[:, None] - onehot) * (1.0 - squashed * squashed)
        grad_logits = slope.astype(jnp.bfloat16)
        row_grad = jnp.dot(grad_logits, unembed, preferred_element_type=jnp.float32)
        grads.append(row_grad.astype(jnp.bfloat16))
        trunk_grad = trunk_grad + row_grad
        unembed_grad = unembed_grad + jnp.dot(grad_logits.T, hidden, preferred_element_type=jnp.float32)
    return jnp.stack(grads), trunk_grad.astype(jnp.bfloat16), unembed_grad
```

```python
import functools

import jax
import jax.numpy as jnp
from jax import lax
from jax.experimental import pallas as pl
from jax.experimental.pallas import tpu as pltpu
from jax.sharding import PartitionSpec as P

soft_cap = 30.0
bf16 = jnp.bfloat16
f32 = jnp.float32
f16 = jnp.float16
VMEM_LIMIT = 60 * 2**20
NX = 3


def params(n=1):
    return pltpu.CompilerParams(
        dimension_semantics=("arbitrary",) * n, vmem_limit_bytes=VMEM_LIMIT
    )


def cost(flops, nbytes):
    return pl.CostEstimate(flops=int(flops), bytes_accessed=int(nbytes), transcendentals=0)


def smem():
    return pl.BlockSpec(memory_space=pltpu.SMEM)


def whole(shape):
    return pl.BlockSpec(shape, lambda *_: (0,) * len(shape))


def scores_kernel(n, pieces, *refs):
    if pieces:
        seq_ref, refs = refs[0], refs[1:]
        parts, (u_ref, o_ref, h_ref, ht_ref) = refs[:n], refs[n:]
        rows = parts[0].shape[0]
    else:
        h_ref, u_ref, o_ref, ht_ref = refs

    @pl.when(pl.program_id(0) == 0)
    def _():
        if pieces:
            for k in range(n):
                at = pl.multiple_of((seq_ref[0] ^ k) * rows, rows)
                h_ref[pl.ds(at, rows), :] = parts[k][...]
        ht_ref[...] = h_ref[...].T

    s = jnp.dot(u_ref[...], ht_ref[...], preferred_element_type=f32)
    o_ref[...] = s.T


def scores_call(seq, hidden, unembed, chunk, block):
    pieces = isinstance(hidden, list)
    rows, width = unembed.shape
    tokens = sum(p.shape[0] for p in hidden) if pieces else hidden.shape[0]
    rows //= NX
    steps = rows // block
    u_spec = pl.BlockSpec((block, width), lambda i: (chunk * steps + i, 0))
    o_spec = pl.BlockSpec((tokens, block), lambda i: (0, i))
    o_shape = jax.ShapeDtypeStruct((tokens, rows), f32)
    est = cost(2 * tokens * rows * width, 2 * rows * width)
    scratch = [pltpu.VMEM((width, tokens), bf16)]
    if pieces:
        return pl.pallas_call(
            functools.partial(scores_kernel, len(hidden), True),
            grid=(steps,),
            in_specs=[smem()] + [whole(p.shape) for p in hidden] + [u_spec],
            out_specs=[o_spec, whole((tokens, width))],
            out_shape=[o_shape, jax.ShapeDtypeStruct((tokens, width), bf16)],
            scratch_shapes=scratch,
            compiler_params=params(),
            cost_estimate=est,
            name="scores_first",
        )(seq, *hidden, unembed)
    return pl.pallas_call(
        functools.partial(scores_kernel, 0, False),
        grid=(steps,),
        in_specs=[whole(hidden.shape), u_spec],
        out_specs=o_spec,
        out_shape=o_shape,
        scratch_shapes=scratch,
        compiler_params=params(),
        cost_estimate=est,
        name="scores_next",
    )(hidden, unembed)


def soften(s):
    squashed = jnp.tanh(s / soft_cap)
    return jnp.exp(soft_cap * squashed), 1.0 - squashed * squashed


def hits(first, targets, shape):
    ids = first + lax.broadcasted_iota(jnp.int32, shape, 1)
    return ids == targets


def numer_kernel(first_ref, s_ref, t_ref, q_ref, stat_ref):
    tokens, rows = s_ref.shape
    sum_e = sum_q = sum_d = 0.0
    step = 128
    for j in range(0, rows, step):
        e, d = soften(s_ref[:, j : j + step])
        hit = hits(first_ref[0] + j, t_ref[...], e.shape)
        q = e * d
        q_ref[:tokens, j : j + step] = jnp.where(hit, 0.0, q).astype(bf16)
        q_ref[tokens:, j : j + step] = jnp.where(hit, 1.0, 0.0).astype(bf16)
        sum_e = sum_e + e
        sum_q = sum_q + jnp.where(hit, q, 0.0)
        sum_d = sum_d + jnp.where(hit, d, 0.0)
    for k, a in enumerate((sum_e, sum_q, sum_d)):
        stat_ref[8 * k : 8 * k + 8, :] = jnp.broadcast_to(
            jnp.sum(a.T, axis=0, keepdims=True), (8, tokens)
        )


def numer_call(first, s, targets):
    tokens, rows = s.shape
    return pl.pallas_call(
        numer_kernel,
        in_specs=[smem(), pl.BlockSpec(memory_space=pltpu.VMEM), pl.BlockSpec(memory_space=pltpu.VMEM)],
        out_specs=[pl.BlockSpec(memory_space=pltpu.VMEM)] * 2,
        out_shape=[
            jax.ShapeDtypeStruct((2 * tokens, rows), bf16),
            jax.ShapeDtypeStruct((24, tokens), f32),
        ],
        compiler_params=pltpu.CompilerParams(vmem_limit_bytes=VMEM_LIMIT),
        cost_estimate=cost(40 * tokens * rows, 8 * tokens * rows),
        name="numer",
    )(first, s, targets)


def rows_kernel(q_ref, u_ref, o_ref):
    o_ref[...] = jnp.dot(q_ref[...], u_ref[...], preferred_element_type=f32)


def rows_call(q, unembed, part, parts, block):
    two, rows = q.shape
    width = unembed.shape[1] // parts
    steps = width // block
    return pl.pallas_call(
        rows_kernel,
        grid=(steps,),
        in_specs=[whole(q.shape), pl.BlockSpec((rows, block), lambda i: (0, part * steps + i))],
        out_specs=pl.BlockSpec((two, block), lambda i: (0, i)),
        out_shape=jax.ShapeDtypeStruct((two, width), f32),
        compiler_params=params(),
        cost_estimate=cost(2 * two * rows * width, 2 * rows * width),
        name="rows",
    )(q, unembed)


def column(row):
    return jnp.broadcast_to(row, (row.shape[1], row.shape[1])).T[:, :1]


def norm_kernel(n, parts, seq_ref, tot_ref, stat_ref, lg_ref, *refs):
    outs = refs[parts:]
    tokens = tot_ref.shape[1]
    rows = tokens // n
    total = tot_ref[...]
    lg = lg_ref[...]
    scale = lg / total
    weight = lg * (stat_ref[8:9, :] / total - stat_ref[16:17, :])
    scale_c, weight_c = column(scale), column(weight)
    sc = outs[-2]
    wc = outs[-1]
    sc[...] = jnp.broadcast_to(scale_c, sc.shape)
    wc[...] = jnp.broadcast_to(weight_c, wc.shape)
    for k in range(n):
        at = pl.multiple_of((seq_ref[0] ^ k) * rows, rows)
        a_s = sc[pl.ds(at, rows), :1]
        a_w = wc[pl.ds(at, rows), :1]
        for p in range(parts):
            width = refs[p].shape[1]
            a = refs[p][pl.ds(at, rows), :]
            u = refs[p][pl.ds(tokens + at, rows), :]
            outs[k][:, p * width : (p + 1) * width] = (a_s * a + a_w * u).astype(bf16)


def norm_call(n, seq, total, stats, loss_grad, sums):
    tokens = total.shape[1]
    width = sum(a.shape[1] for a in sums)
    vm = pl.BlockSpec(memory_space=pltpu.VMEM)
    return pl.pallas_call(
        functools.partial(norm_kernel, n, len(sums)),
        in_specs=[smem()] + [vm] * (3 + len(sums)),
        out_specs=[vm] * n,
        out_shape=[jax.ShapeDtypeStruct((tokens // n, width), bf16)] * n,
        scratch_shapes=[pltpu.VMEM((tokens, 128), f32)] * 2,
        compiler_params=pltpu.CompilerParams(vmem_limit_bytes=VMEM_LIMIT),
        cost_estimate=cost(4 * tokens * width, 10 * tokens * width),
        name="norm",
    )(seq, total, stats, loss_grad, *sums)


def grads_kernel(first_ref, s_ref, t_ref, tot_ref, lg_ref, g_ref):
    tokens, rows = s_ref.shape
    inv = column(1.0 / tot_ref[...])
    lg = column(lg_ref[...])
    step = 128
    for j in range(0, rows, step):
        e, d = soften(s_ref[:, j : j + step])
        hit = hits(first_ref[0] + j, t_ref[...], e.shape)
        g_ref[:, j : j + step] = (
            lg * (e * inv - jnp.where(hit, 1.0, 0.0)) * d
        ).astype(bf16)


def grads_call(first, s, targets, total, loss_grad):
    vm = pl.BlockSpec(memory_space=pltpu.VMEM)
    return pl.pallas_call(
        grads_kernel,
        in_specs=[smem()] + [vm] * 4,
        out_specs=vm,
        out_shape=jax.ShapeDtypeStruct(s.shape, bf16),
        compiler_params=pltpu.CompilerParams(vmem_limit_bytes=VMEM_LIMIT),
        cost_estimate=cost(40 * s.size, 6 * s.size),
        name="grads",
    )(first, s, targets, total, loss_grad)


def weight_kernel(head_ref, g0_ref, g1_ref, h0_ref, h1_ref, *refs):
    o_ref, g_ref, h_ref = refs[-3:]
    tokens = h0_ref.shape[0]
    mine = pl.multiple_of(head_ref[0] * tokens, tokens)
    other = pl.multiple_of((1 - head_ref[0]) * tokens, tokens)

    @pl.when(pl.program_id(0) == 0)
    def _():
        h_ref[pl.ds(mine, tokens), :] = h0_ref[...]
        h_ref[pl.ds(other, tokens), :] = h1_ref[...]

    g_ref[pl.ds(mine, tokens), :] = g0_ref[...]
    g_ref[pl.ds(other, tokens), :] = g1_ref[...]
    o_ref[...] = lax.dot_general(
        g_ref[...], h_ref[...], (((0,), (0,)), ((), ())), preferred_element_type=f32
    )


def weight_call(head, g0, g1, h0, h1, part, parts, block, into):
    tokens, rows = g0.shape
    width = h0.shape[1]
    steps = rows // parts // block
    g_spec = pl.BlockSpec((tokens, block), lambda i: (0, part * steps + i))
    operands = [head, g0, g1, h0, h1]
    specs = [smem(), g_spec, g_spec, whole(h0.shape), whole(h1.shape)]
    alias = {}
    if into is not None:
        operands.append(into)
        specs.append(pl.BlockSpec(memory_space=pl.ANY))
        alias = {5: 0}
    return pl.pallas_call(
        weight_kernel,
        grid=(steps,),
        in_specs=specs,
        out_specs=pl.BlockSpec((block, width), lambda i: (part * steps + i, 0)),
        out_shape=jax.ShapeDtypeStruct((rows, width), f32),
        scratch_shapes=[pltpu.VMEM((2 * tokens, block), bf16), pltpu.VMEM((2 * tokens, width), bf16)],
        input_output_aliases=alias,
        compiler_params=params(),
        cost_estimate=cost(4 * tokens * rows * width / parts, 4 * rows * width / parts),
        name="weight",
    )(*operands)


def swap(x, axis, mask, size):
    return lax.ppermute(x, axis, [(i, i ^ mask) for i in range(size)])


def fast(n, trunk, branch, unembed, targets, loss_grad):
    block_rows = unembed.shape[0]
    seq_index = lax.axis_index("seq")
    seq = seq_index.astype(jnp.int32)[None]
    head = lax.axis_index("head").astype(jnp.int32)[None]
    first = (seq_index * block_rows).astype(jnp.int32)[None]
    targets_c = jnp.broadcast_to(targets[0][:, None], (targets.shape[1], 128))
    hidden = (trunk.astype(f32) + branch[0].astype(f32)).astype(bf16)

    pieces = [None] * n
    pieces[0] = hidden
    for k in (k for k in (2, 6, 4) if k < n):
        pieces[k] = swap(hidden, "seq", k, n)
    for k in (k for k in (0, 2, 6, 4) if k < n):
        pieces[k + 1] = swap(pieces[k], "seq", 1, n)

    block = block_rows // 6
    mine, theirs = [], []
    whole_hidden = None
    for c in range(NX):
        if c == 0:
            s, whole_hidden = scores_call(seq, pieces, unembed, c, block)
        else:
            s = scores_call(seq, whole_hidden, unembed, c, block)
        s = s.astype(f16)
        mine.append(s)
        theirs.append(swap(s, "mp", 1, 2))
    other_hidden = swap(whole_hidden, "head", 1, 2)
    scores = jnp.concatenate([a.astype(f32) + b.astype(f32) for a, b in zip(mine, theirs)], axis=1)

    q, stats = numer_call(first, scores, targets_c)
    total = stats[:1]
    sums = []
    parts = 2
    masks = [1 << i for i in range(n.bit_length() - 1)]
    for mask in masks:
        total = total + swap(total, "seq", mask, n)
    for p in range(parts):
        sums.append(rows_call(q, unembed, p, parts, 512))
    blocks = norm_call(n, seq, total, stats, loss_grad, sums)

    got = []
    for k in (k for k in (2, 6, 4, 0) if k < n):
        theirs = swap(blocks[k + 1], "seq", 1, n)
        both = blocks[k].astype(f32) + theirs.astype(f32)
        if k:
            both = swap(both.astype(bf16), "seq", k, n).astype(f32)
        got.append(both)
    row_grad = functools.reduce(lambda a, b: a + b, got)

    g = grads_call(first, scores, targets_c, total, loss_grad)
    g_other = swap(g, "head", 1, 2)
    d_unembed = None
    for p in range(3):
        d_unembed = weight_call(head, g, g_other, whole_hidden, other_hidden, p, 3, 256, d_unembed)

    d_trunk = row_grad + swap(row_grad, "head", 1, 2)
    return (row_grad.astype(bf16)[None], d_trunk.astype(bf16), d_unembed)


def general(trunk, branch, unembed, targets, loss_grad):
    block_rows = unembed.shape[0]
    hidden = (trunk.astype(f32) + branch[0].astype(f32)).astype(bf16)
    gathered = lax.all_gather(hidden, "seq", axis=0, tiled=True)
    seq_index = lax.axis_index("seq")
    scores = lax.psum(
        lax.dot_general(unembed, gathered, (((1,), (1,)), ((), ())), preferred_element_type=f32),
        "mp",
    )
    exponent, slope = soften(scores)
    totals = lax.psum(jnp.sum(exponent, axis=0), "seq")
    vocab_ids = seq_index * block_rows + lax.iota(jnp.int32, block_rows)
    onehot = (vocab_ids[:, None] == targets[0][None, :]).astype(f32)
    grad_logits = (
        loss_grad[0][None, :] * (exponent / totals[None, :] - onehot) * slope
    ).astype(bf16)
    row_grad = lax.psum_scatter(
        lax.dot_general(grad_logits, unembed, (((0,), (0,)), ((), ())), preferred_element_type=f32),
        "seq",
        scatter_dimension=0,
        tiled=True,
    )
    weight_grad = jnp.dot(grad_logits, gathered, preferred_element_type=f32)
    trunk_sum, unembed_sum = lax.psum((row_grad, weight_grad), "head")
    return (row_grad.astype(bf16)[None], trunk_sum.astype(bf16), unembed_sum)


def solution(mesh):
    in_specs = (
        P("seq", "mp"),
        P("head", "seq", "mp"),
        P("seq", "mp"),
        P("head", None),
        P("head", None),
    )
    out_specs = (P("head", "seq", "mp"), P("seq", "mp"), P("seq", "mp"))
    n = mesh.shape["seq"]
    pairs = mesh.shape["head"] == 2 and mesh.shape["mp"] == 2
    body = functools.partial(fast, n) if pairs and n in (2, 4, 8) else general
    return jax.shard_map(body, mesh=mesh, in_specs=in_specs, out_specs=out_specs, check_vma=False)
```

```python
import functools

import jax
import jax.numpy as jnp
from jax import lax
from jax.experimental import pallas as pl
from jax.experimental.pallas import tpu as pltpu
from jax.sharding import PartitionSpec as P


soft_cap = 30.0
bf16 = jnp.bfloat16
f32 = jnp.float32
f16 = jnp.float16
MIB = 2**20


def params(n, limit=12):
    return pltpu.CompilerParams(
        dimension_semantics=("arbitrary",) * n if n else None, vmem_limit_bytes=limit * MIB
    )


def cost(flops, nbytes):
    return pl.CostEstimate(flops=int(flops), bytes_accessed=int(nbytes), transcendentals=0)


def smem():
    return pl.BlockSpec(memory_space=pltpu.SMEM)


def vmem():
    return pl.BlockSpec(memory_space=pltpu.VMEM)


def stage_kernel(ids_ref, u_ref, o_ref, sem):
    copy = pltpu.make_async_copy(u_ref, o_ref, sem)
    copy.start()
    copy.wait()


def stage_call(ids, unembed):
    return pl.pallas_call(
        stage_kernel,
        in_specs=[smem(), pl.BlockSpec(memory_space=pltpu.HBM)],
        out_specs=vmem(),
        out_shape=jax.ShapeDtypeStruct(unembed.shape, unembed.dtype),
        scratch_shapes=[pltpu.SemaphoreType.DMA],
        compiler_params=params(0, 28),
        cost_estimate=cost(unembed.size, 4 * unembed.size),
        name="stage",
    )(ids, unembed)


def first_kernel(n, ids_ref, *refs):
    parts, (u_ref, o_ref, h_ref, ht_ref) = refs[:n], refs[n:]
    rows = parts[0].shape[0]
    for k in range(n):
        at = pl.multiple_of((ids_ref[0] ^ k) * rows, rows)
        h_ref[pl.ds(at, rows), :] = parts[k][...]
    ht_ref[...] = h_ref[...].T
    count = o_ref.shape[1]
    o_ref[...] = jnp.dot(u_ref[:count, :], ht_ref[...], preferred_element_type=f32).T


def next_kernel(start, ht_ref, u_ref, o_ref):
    count = o_ref.shape[1]
    o_ref[...] = jnp.dot(
        u_ref[start : start + count, :], ht_ref[...], preferred_element_type=f32
    ).T


def first_call(ids, pieces, unembed, count):
    width = unembed.shape[1]
    tokens = sum(p.shape[0] for p in pieces)
    return pl.pallas_call(
        functools.partial(first_kernel, len(pieces)),
        in_specs=[smem()] + [vmem()] * (len(pieces) + 1),
        out_specs=[vmem()] * 3,
        out_shape=[
            jax.ShapeDtypeStruct((tokens, count), f32),
            jax.ShapeDtypeStruct((tokens, width), bf16),
            jax.ShapeDtypeStruct((width, tokens), bf16),
        ],
        compiler_params=params(0),
        cost_estimate=cost(2 * tokens * count * width, 2 * count * width),
        name="scores_first",
    )(ids, *pieces, unembed)


def next_call(turned, unembed, start, count):
    width, tokens = turned.shape
    return pl.pallas_call(
        functools.partial(next_kernel, start),
        in_specs=[vmem()] * 2,
        out_specs=vmem(),
        out_shape=jax.ShapeDtypeStruct((tokens, count), f32),
        compiler_params=params(0),
        cost_estimate=cost(2 * tokens * count * width, 2 * count * width),
        name="scores_next",
    )(turned, unembed)


def soften(s):
    squashed = jnp.tanh(s * (1.0 / soft_cap))
    return jnp.exp(soft_cap * squashed), 1.0 - squashed * squashed


def hits(first, targets, shape):
    ids = first + lax.broadcasted_iota(jnp.int32, shape, 1)
    return ids == targets


def column(row):
    return jnp.broadcast_to(row, (row.shape[1], row.shape[1])).T[:, :1]


def numer_kernel(start, ids_ref, s_ref, t_ref, *refs):
    q_ref, tot_ref, stat_ref = refs[-3:]
    tokens, rows = s_ref.shape
    targets = column(t_ref[...])
    sum_e = sum_q = sum_d = 0.0
    step = 128
    for j in range(0, rows, step):
        e, d = soften(s_ref[:, j : j + step])
        hit = hits(ids_ref[2] + (start + j), targets, e.shape)
        q = e * d
        q_ref[:tokens, j : j + step] = jnp.where(hit, 0.0, q).astype(bf16)
        q_ref[tokens:, j : j + step] = jnp.where(hit, 1.0, 0.0).astype(bf16)
        sum_e = sum_e + e
        sum_q = sum_q + jnp.where(hit, q, 0.0)
        sum_d = sum_d + jnp.where(hit, d, 0.0)
    tot, sq, sd = (jnp.sum(a.T, axis=0, keepdims=True) for a in (sum_e, sum_q, sum_d))
    if len(refs) > 3:
        tot = tot + refs[0][...]
        sq = sq + refs[1][:1, :]
        sd = sd + refs[1][1:2, :]
    tot_ref[...] = tot
    stat_ref[:1, :] = sq
    stat_ref[1:2, :] = sd


def numer_call(start, ids, s, targets, so_far):
    tokens, rows = s.shape
    return pl.pallas_call(
        functools.partial(numer_kernel, start),
        in_specs=[smem()] + [vmem()] * (2 + len(so_far)),
        out_specs=[vmem()] * 3,
        out_shape=[
            jax.ShapeDtypeStruct((2 * tokens, rows), bf16),
            jax.ShapeDtypeStruct((1, tokens), f32),
            jax.ShapeDtypeStruct((2, tokens), f32),
        ],
        compiler_params=params(0),
        cost_estimate=cost(40 * tokens * rows, 8 * tokens * rows),
        name="numer",
    )(ids, s, targets, *so_far)


def rows_kernel(start, block, count, *refs):
    qs, (u_ref, o_ref, q_ref) = refs[:count], refs[count:]

    @pl.when(pl.program_id(0) == 0)
    def _():
        at = 0
        for q in qs:
            q_ref[:, at : at + q.shape[1]] = q[...]
            at += q.shape[1]

    cols = pl.ds(pl.multiple_of(start + pl.program_id(0) * block, block), block)
    o_ref[...] = jnp.dot(q_ref[...], u_ref[:, cols], preferred_element_type=f32)


def rows_call(qs, unembed, start, width, block):
    rows = unembed.shape[0]
    two = qs[0].shape[0]
    return pl.pallas_call(
        functools.partial(rows_kernel, start, block, len(qs)),
        grid=(width // block,),
        in_specs=[vmem()] * (len(qs) + 1),
        out_specs=pl.BlockSpec((two, block), lambda i: (0, i)),
        out_shape=jax.ShapeDtypeStruct((two, width), f32),
        scratch_shapes=[pltpu.VMEM((two, rows), bf16)],
        compiler_params=params(1),
        cost_estimate=cost(2 * two * rows * width, 2 * rows * width),
        name="rows",
    )(*qs, unembed)


def norm_kernel(n, parts, ids_ref, tot_ref, stat_ref, lg_ref, *refs):
    outs = refs[parts : parts + n]
    sc, wc = refs[parts + n :]
    tokens = tot_ref.shape[1]
    rows = tokens // n
    total = tot_ref[...]
    lg = lg_ref[...]
    sc[...] = jnp.broadcast_to(lg / total, (tokens, tokens)).T
    weight = lg * (stat_ref[:1, :] / total - stat_ref[1:2, :])
    wc[...] = jnp.broadcast_to(weight, (tokens, tokens)).T
    for k in range(n):
        at = pl.multiple_of((ids_ref[0] ^ k) * rows, rows)
        a_s = sc[pl.ds(at, rows), :1]
        a_w = wc[pl.ds(at, rows), :1]
        col = 0
        for p in range(parts):
            width = refs[p].shape[1]
            a = refs[p][pl.ds(at, rows), :]
            u = refs[p][pl.ds(tokens + at, rows), :]
            outs[k][:, col : col + width] = (a_s * a + a_w * u).astype(bf16)
            col += width


def norm_call(n, ids, total, stats, loss_grad, sums):
    tokens = total.shape[1]
    width = sum(a.shape[1] for a in sums)
    return pl.pallas_call(
        functools.partial(norm_kernel, n, len(sums)),
        in_specs=[smem()] + [vmem()] * (3 + len(sums)),
        out_specs=[vmem()] * n,
        out_shape=[jax.ShapeDtypeStruct((tokens // n, width), bf16)] * n,
        scratch_shapes=[pltpu.VMEM((tokens, tokens), f32)] * 2,
        compiler_params=params(0),
        cost_estimate=cost(4 * tokens * width, 10 * tokens * width),
        name="norm",
    )(ids, total, stats, loss_grad, *sums)


def grads_kernel(count, ids_ref, t_ref, tot_ref, lg_ref, *refs):
    g_ref = refs[count]
    inv = column(1.0 / tot_ref[...])
    lg = column(lg_ref[...])
    targets = column(t_ref[...])
    step = 128
    at = 0
    for s_ref in refs[:count]:
        for j in range(0, s_ref.shape[1], step):
            e, d = soften(s_ref[:, j : j + step])
            hit = hits(ids_ref[2] + at, targets, e.shape)
            p = jnp.where(hit, e * inv - 1.0, e * inv)
            g_ref[:, at : at + step] = (lg * p * d).astype(bf16)
            at += step


def grads_call(ids, scores, targets, total, loss_grad):
    tokens = total.shape[1]
    rows = sum(s.shape[1] for s in scores)
    return pl.pallas_call(
        functools.partial(grads_kernel, len(scores)),
        in_specs=[smem()] + [vmem()] * (3 + len(scores)),
        out_specs=vmem(),
        out_shape=jax.ShapeDtypeStruct((tokens, rows), bf16),
        compiler_params=params(0),
        cost_estimate=cost(40 * tokens * rows, 6 * tokens * rows),
        name="grads",
    )(ids, targets, total, loss_grad, *scores)


def weight_kernel(ids_ref, g0_ref, g1_ref, h0_ref, h1_ref, *refs):
    o_ref, g_ref, h_ref = refs[-3:]
    tokens = h0_ref.shape[0]
    mine = pl.multiple_of(ids_ref[1] * tokens, tokens)
    other = pl.multiple_of((1 - ids_ref[1]) * tokens, tokens)

    @pl.when(pl.program_id(0) == 0)
    def _():
        h_ref[pl.ds(mine, tokens), :] = h0_ref[...]
        h_ref[pl.ds(other, tokens), :] = h1_ref[...]

    g_ref[pl.ds(mine, tokens), :] = g0_ref[...]
    g_ref[pl.ds(other, tokens), :] = g1_ref[...]
    o_ref[...] = lax.dot_general(
        g_ref[...], h_ref[...], (((0,), (0,)), ((), ())), preferred_element_type=f32
    )


def weight_call(ids, g0, g1, h0, h1, start, count, block, into):
    tokens, rows = g0.shape
    width = h0.shape[1]
    g_spec = pl.BlockSpec((tokens, block), lambda i: (0, start // block + i))
    operands = [ids, g0, g1, h0, h1]
    specs = [smem(), g_spec, g_spec, vmem(), vmem()]
    alias = {}
    if into is not None:
        operands.append(into)
        specs.append(pl.BlockSpec(memory_space=pl.ANY))
        alias = {5: 0}
    return pl.pallas_call(
        weight_kernel,
        grid=(count // block,),
        in_specs=specs,
        out_specs=pl.BlockSpec((block, width), lambda i: (start // block + i, 0)),
        out_shape=jax.ShapeDtypeStruct((rows, width), f32),
        scratch_shapes=[pltpu.VMEM((2 * tokens, block), bf16), pltpu.VMEM((2 * tokens, width), bf16)],
        input_output_aliases=alias,
        compiler_params=params(1, 24),
        cost_estimate=cost(4 * tokens * count * width, 4 * count * width),
        name="weight",
    )(*operands)


def swap(x, axis, mask, size):
    return lax.ppermute(x, axis, [(i, i ^ mask) for i in range(size)])


def split(total, unit):
    tiles = total // unit
    sizes = [1, (tiles - 2) // 2, (tiles - 3) // 2, 2]
    starts = [sum(sizes[:i]) for i in range(len(sizes))]
    return [(a * unit, c * unit) for a, c in zip(starts, sizes)]


def thirds(total, unit):
    tiles = total // unit
    sizes = [(tiles + 2) // 3, (tiles + 1) // 3, tiles // 3]
    starts = [sum(sizes[:i]) for i in range(3)]
    return [(a * unit, c * unit) for a, c in zip(starts, sizes)]


def fast(n, trunk, branch, unembed, targets, loss_grad):
    block_rows, width = unembed.shape
    seq_index = lax.axis_index("seq")
    ids = jnp.stack([seq_index, lax.axis_index("head"), seq_index * block_rows]).astype(jnp.int32)
    hidden = (trunk.astype(f32) + branch[0].astype(f32)).astype(bf16)
    far = [k for k in (2, 6, 4) if k < n]

    pieces = [None] * n
    pieces[0] = hidden
    for k in far:
        pieces[k] = swap(hidden, "seq", k, n)
    for k in [0] + far:
        pieces[k + 1] = swap(pieces[k], "seq", 1, n)

    unembed = stage_call(ids, unembed)
    chunks = split(block_rows, 256)
    scores, qs, so_far = [], [], []
    for c, (start, count) in enumerate(chunks):
        if c == 0:
            s, all_hidden, turned = first_call(ids, pieces, unembed, count)
        else:
            s = next_call(turned, unembed, start, count)
        s = s.astype(f16)
        scores.append(s.astype(f32) + swap(s, "mp", 1, 2).astype(f32))
    other_hidden = swap(all_hidden, "head", 1, 2)
    for c, (start, count) in enumerate(chunks):
        q, *so_far = numer_call(start, ids, scores[c], targets, so_far)
        qs.append(q)
    total, stats = so_far

    for i in range(n.bit_length() - 1):
        total = total + swap(total, "seq", 1 << i, n)
    sums = []
    for start, count in thirds(width, 512):
        sums.append(rows_call(qs, unembed, start, count, 512))
    blocks = norm_call(n, ids, total, stats, loss_grad, sums)

    got = []
    for k in far + [0]:
        theirs = swap(blocks[k + 1], "seq", 1, n)
        both = blocks[k].astype(f32) + theirs.astype(f32)
        if k:
            both = swap(both.astype(bf16), "seq", k, n).astype(f32)
        got.append(both)
    row_grad = functools.reduce(lambda a, b: a + b, got)

    g = grads_call(ids, scores, targets, total, loss_grad)
    g_other = swap(g, "head", 1, 2)
    d_unembed = None
    for start, count in thirds(block_rows, 256):
        d_unembed = weight_call(
            ids, g, g_other, all_hidden, other_hidden, start, count, 256, d_unembed
        )

    d_trunk = row_grad + swap(row_grad, "head", 1, 2)
    return (row_grad.astype(bf16)[None], d_trunk.astype(bf16), d_unembed)


def general(trunk, branch, unembed, targets, loss_grad):
    block_rows = unembed.shape[0]
    hidden = (trunk.astype(f32) + branch[0].astype(f32)).astype(bf16)
    gathered = lax.all_gather(hidden, "seq", axis=0, tiled=True)
    seq_index = lax.axis_index("seq")
    scores = lax.psum(
        lax.dot_general(unembed, gathered, (((1,), (1,)), ((), ())), preferred_element_type=f32),
        "mp",
    )
    exponent, slope = soften(scores)
    totals = lax.psum(jnp.sum(exponent, axis=0), "seq")
    vocab_ids = seq_index * block_rows + lax.iota(jnp.int32, block_rows)
    onehot = (vocab_ids[:, None] == targets[0][None, :]).astype(f32)
    grad_logits = (
        loss_grad[0][None, :] * (exponent / totals[None, :] - onehot) * slope
    ).astype(bf16)
    row_grad = lax.psum_scatter(
        lax.dot_general(grad_logits, unembed, (((0,), (0,)), ((), ())), preferred_element_type=f32),
        "seq",
        scatter_dimension=0,
        tiled=True,
    )
    weight_grad = jnp.dot(grad_logits, gathered, preferred_element_type=f32)
    trunk_sum, unembed_sum = lax.psum((row_grad, weight_grad), "head")
    return (row_grad.astype(bf16)[None], trunk_sum.astype(bf16), unembed_sum)


def solution(mesh):
    in_specs = (
        P("seq", "mp"),
        P("head", "seq", "mp"),
        P("seq", "mp"),
        P("head", None),
        P("head", None),
    )
    out_specs = (P("head", "seq", "mp"), P("seq", "mp"), P("seq", "mp"))
    n = mesh.shape["seq"]
    if mesh.shape["head"] == 2 and mesh.shape["mp"] == 2 and n == 8:

        def body(*args):
            return fast(n, *args)
    else:
        body = general
    step = jax.shard_map(body, mesh=mesh, in_specs=in_specs, out_specs=out_specs, check_vma=False)
    if body is general:
        return step
    return step
```

```python
import functools

import jax
import jax.numpy as jnp
from jax import lax
from jax.experimental import pallas as pl
from jax.experimental.pallas import tpu as pltpu
from jax.sharding import PartitionSpec as P


soft_cap = 30.0
bf16 = jnp.bfloat16
f32 = jnp.float32
f16 = jnp.float16
MIB = 2**20
STAGE_LIMIT = 42


def params(n, limit=12):
    return pltpu.CompilerParams(
        dimension_semantics=("arbitrary",) * n if n else None, vmem_limit_bytes=limit * MIB
    )


def cost(flops, nbytes):
    return pl.CostEstimate(flops=int(flops), bytes_accessed=int(nbytes), transcendentals=0)


def smem():
    return pl.BlockSpec(memory_space=pltpu.SMEM)


def vmem():
    return pl.BlockSpec(memory_space=pltpu.VMEM)


def stage_kernel(start, ids_ref, u_ref, o_ref, sem):
    copy = pltpu.make_async_copy(u_ref.at[pl.ds(start, o_ref.shape[0])], o_ref, sem)
    copy.start()
    copy.wait()


def stage_call(ids, unembed, start, count):
    shape = (count, unembed.shape[1])
    return pl.pallas_call(
        functools.partial(stage_kernel, start),
        in_specs=[smem(), pl.BlockSpec(memory_space=pltpu.HBM)],
        out_specs=vmem(),
        out_shape=jax.ShapeDtypeStruct(shape, unembed.dtype),
        scratch_shapes=[pltpu.SemaphoreType.DMA],
        compiler_params=params(0, STAGE_LIMIT),
        cost_estimate=cost(count * shape[1], 4 * count * shape[1]),
        name="stage",
    )(ids, unembed)


def first_kernel(n, ids_ref, *refs):
    parts, (u_ref, o_ref, h_ref, ht_ref) = refs[:n], refs[n:]
    rows = parts[0].shape[0]
    for k in range(n):
        at = pl.multiple_of((ids_ref[0] ^ k) * rows, rows)
        h_ref[pl.ds(at, rows), :] = parts[k][...]
    ht_ref[...] = h_ref[...].T
    u = u_ref[: o_ref.shape[1], :]
    o_ref[...] = jnp.dot(u, ht_ref[...], preferred_element_type=f32).T


def next_kernel(start, ht_ref, u_ref, o_ref):
    u = u_ref[start : start + o_ref.shape[1], :]
    o_ref[...] = jnp.dot(u, ht_ref[...], preferred_element_type=f32).T


def first_call(ids, pieces, unembed, count):
    width = unembed.shape[1]
    tokens = sum(p.shape[0] for p in pieces)
    return pl.pallas_call(
        functools.partial(first_kernel, len(pieces)),
        in_specs=[smem()] + [vmem()] * (len(pieces) + 1),
        out_specs=[vmem()] * 3,
        out_shape=[
            jax.ShapeDtypeStruct((tokens, count), f32),
            jax.ShapeDtypeStruct((tokens, width), bf16),
            jax.ShapeDtypeStruct((width, tokens), bf16),
        ],
        compiler_params=params(0),
        cost_estimate=cost(2 * tokens * count * width, 2 * count * width),
        name="scores_first",
    )(ids, *pieces, unembed)


def next_call(turned, unembed, start, count):
    width, tokens = turned.shape
    return pl.pallas_call(
        functools.partial(next_kernel, start),
        in_specs=[vmem()] * 2,
        out_specs=vmem(),
        out_shape=jax.ShapeDtypeStruct((tokens, count), f32),
        compiler_params=params(0),
        cost_estimate=cost(2 * tokens * count * width, 2 * count * width),
        name="scores_next",
    )(turned, unembed)


def soften(s):
    squashed = jnp.tanh(s * (1.0 / soft_cap))
    return jnp.exp(soft_cap * squashed), 1.0 - squashed * squashed


def hits(first, targets, shape):
    ids = first + lax.broadcasted_iota(jnp.int32, shape, 1)
    return ids == targets


def column(row):
    return jnp.broadcast_to(row, (row.shape[1], row.shape[1])).T[:, :1]


def numer_kernel(start, ids_ref, s_ref, t_ref, *refs):
    q_ref, tot_ref, stat_ref = refs[-3:]
    tokens, rows = s_ref.shape
    targets = column(t_ref[...])
    sum_e = sum_q = sum_d = 0.0
    step = 128
    for j in range(0, rows, step):
        e, d = soften(s_ref[:, j : j + step])
        hit = hits(ids_ref[2] + (start + j), targets, e.shape)
        q = e * d
        q_ref[:tokens, j : j + step] = jnp.where(hit, 0.0, q).astype(bf16)
        q_ref[tokens:, j : j + step] = jnp.where(hit, 1.0, 0.0).astype(bf16)
        sum_e = sum_e + e
        sum_q = sum_q + jnp.where(hit, q, 0.0)
        sum_d = sum_d + jnp.where(hit, d, 0.0)
    tot, sq, sd = (jnp.sum(a.T, axis=0, keepdims=True) for a in (sum_e, sum_q, sum_d))
    if len(refs) > 3:
        tot = tot + refs[0][...]
        sq = sq + refs[1][:1, :]
        sd = sd + refs[1][1:2, :]
    tot_ref[...] = tot
    stat_ref[:1, :] = sq
    stat_ref[1:2, :] = sd


def numer_call(start, ids, s, targets, so_far):
    tokens, rows = s.shape
    return pl.pallas_call(
        functools.partial(numer_kernel, start),
        in_specs=[smem()] + [vmem()] * (2 + len(so_far)),
        out_specs=[vmem()] * 3,
        out_shape=[
            jax.ShapeDtypeStruct((2 * tokens, rows), bf16),
            jax.ShapeDtypeStruct((1, tokens), f32),
            jax.ShapeDtypeStruct((2, tokens), f32),
        ],
        compiler_params=params(0),
        cost_estimate=cost(40 * tokens * rows, 8 * tokens * rows),
        name="numer",
    )(ids, s, targets, *so_far)


def rows_kernel(block, first, *refs):
    *q_refs, u_ref, o_ref = refs
    step = pl.program_id(0) * block
    cols = pl.ds(pl.multiple_of(first + step, block), block)
    total, row = None, 0
    for q_ref in q_refs:
        count = q_ref.shape[1]
        part = jnp.dot(q_ref[...], u_ref[row : row + count, cols], preferred_element_type=f32)
        total = part if total is None else total + part
        row += count
    o_ref[...] = total


def rows_call(qs, unembed, first, width, block):
    two = qs[0].shape[0]
    rows = sum(q.shape[1] for q in qs)
    return pl.pallas_call(
        functools.partial(rows_kernel, block, first),
        grid=(width // block,),
        in_specs=[vmem()] * (len(qs) + 1),
        out_specs=pl.BlockSpec((two, block), lambda i: (0, i)),
        out_shape=jax.ShapeDtypeStruct((two, width), f32),
        compiler_params=params(1),
        cost_estimate=cost(2 * two * rows * width, 2 * rows * width),
        name="rows",
    )(*qs, unembed)


def norm_kernel(n, groups, ids_ref, tot_ref, stat_ref, lg_ref, *refs):
    early, late, refs = refs[:2], refs[2:4], refs[4:]
    keep, send = refs[: n // 2], refs[n // 2 : n // 2 + len(groups)]
    sc, wc = refs[-2:]
    tokens = tot_ref.shape[1]
    rows = tokens // n
    total = tot_ref[...]
    lg = lg_ref[...]
    sc[...] = jnp.broadcast_to(lg / total, (tokens, tokens)).T
    weight = lg * (stat_ref[:1, :] / total - stat_ref[1:2, :])
    wc[...] = jnp.broadcast_to(weight, (tokens, tokens)).T

    def block(k, ref, row):
        at = pl.multiple_of((ids_ref[0] ^ k) * rows, rows)
        scale = sc[pl.ds(at, rows), :1]
        weight = wc[pl.ds(at, rows), :1]
        col = 0
        for x, y in zip(early, late):
            cols = slice(col, col + x.shape[1])
            a = x[pl.ds(at, rows), :] + y[pl.ds(at, rows), :]
            u = x[pl.ds(tokens + at, rows), :] + y[pl.ds(tokens + at, rows), :]
            ref[row : row + rows, cols] = (scale * a + weight * u).astype(ref.dtype)
            col += x.shape[1]

    for ref, group in zip(send, groups):
        for i, k in enumerate(group):
            block(k + 1, ref, i * rows)
    for k in range(0, n, 2):
        block(k, keep[k // 2], 0)


def norm_call(n, groups, ids, total, stats, loss_grad, sums):
    tokens = total.shape[1]
    width = 2 * sums[0].shape[1]
    rows = tokens // n
    return pl.pallas_call(
        functools.partial(norm_kernel, n, groups),
        in_specs=[smem()] + [vmem()] * (3 + len(sums)),
        out_specs=[vmem()] * (n // 2 + len(groups)),
        out_shape=[jax.ShapeDtypeStruct((rows, width), f32)] * (n // 2)
        + [jax.ShapeDtypeStruct((rows * len(g), width), bf16) for g in groups],
        scratch_shapes=[pltpu.VMEM((tokens, tokens), f32)] * 2,
        compiler_params=params(0),
        cost_estimate=cost(4 * tokens * width, 10 * tokens * width),
        name="norm",
    )(ids, total, stats, loss_grad, *sums)


def grads_kernel(count, ids_ref, t_ref, tot_ref, lg_ref, *refs):
    g_ref = refs[count]
    inv = column(1.0 / tot_ref[...])
    lg = column(lg_ref[...])
    targets = column(t_ref[...])
    step = 128
    at = 0
    for s_ref in refs[:count]:
        for j in range(0, s_ref.shape[1], step):
            e, d = soften(s_ref[:, j : j + step])
            hit = hits(ids_ref[2] + at, targets, e.shape)
            p = jnp.where(hit, e * inv - 1.0, e * inv)
            g_ref[:, at : at + step] = (lg * p * d).astype(bf16)
            at += step


def grads_call(ids, scores, targets, total, loss_grad):
    tokens = total.shape[1]
    rows = sum(s.shape[1] for s in scores)
    return pl.pallas_call(
        functools.partial(grads_kernel, len(scores)),
        in_specs=[smem()] + [vmem()] * (3 + len(scores)),
        out_specs=vmem(),
        out_shape=jax.ShapeDtypeStruct((tokens, rows), bf16),
        compiler_params=params(0),
        cost_estimate=cost(40 * tokens * rows, 6 * tokens * rows),
        name="grads",
    )(ids, targets, total, loss_grad, *scores)


def weight_kernel(first, start, block, ids_ref, *refs):
    g0_ref, g1_ref, refs = refs[0], refs[1], refs[2:]
    if first:
        h0_ref, h1_ref, o_ref, h_ref, g_ref, r_ref, sem = refs
    else:
        h_ref, _, o_ref, g_ref, r_ref, sem = refs
    tokens, count = g0_ref.shape[0], g_ref.shape[1]
    mine = pl.multiple_of(ids_ref[1] * tokens, tokens)
    other = pl.multiple_of((1 - ids_ref[1]) * tokens, tokens)
    if first:
        h_ref[pl.ds(mine, tokens), :] = h0_ref[...]
        h_ref[pl.ds(other, tokens), :] = h1_ref[...]
    g_ref[pl.ds(mine, tokens), :] = g0_ref[:, start : start + count]
    g_ref[pl.ds(other, tokens), :] = g1_ref[:, start : start + count]
    turned = g_ref[...].T
    copies = []
    part = r_ref.shape[2]
    across = h_ref.shape[1] // part
    for i in range(r_ref.shape[0]):
        row, col = i // across * block, i % across * part
        r_ref[i] = jnp.dot(
            turned[row : row + block, :],
            h_ref[:, col : col + part],
            preferred_element_type=f32,
        )
        copies.append(
            pltpu.make_async_copy(
                r_ref.at[i],
                o_ref.at[pl.ds(start + row, block), pl.ds(col, part)],
                sem.at[i],
            )
        )
        copies[-1].start()
    for copy in copies:
        copy.wait()


def weight_call(ids, g0, g1, hs, start, count, block, into):
    tokens, rows = g0.shape
    width = hs[0].shape[1]
    hbm = pl.BlockSpec(memory_space=pltpu.HBM)
    first = into is None
    operands = [ids, g0, g1, *hs] + ([] if first else [into])
    specs = [smem()] + [vmem()] * (2 + len(hs)) + ([] if first else [hbm])
    out_specs = [hbm] + ([vmem()] if first else [])
    out_shape = [jax.ShapeDtypeStruct((rows, width), f32)]
    if first:
        out_shape.append(jax.ShapeDtypeStruct((2 * tokens, width), bf16))
    across = 4
    steps = count // block * across
    return pl.pallas_call(
        functools.partial(weight_kernel, first, start, block),
        in_specs=specs,
        out_specs=out_specs,
        out_shape=out_shape,
        scratch_shapes=[
            pltpu.VMEM((2 * tokens, count), bf16),
            pltpu.VMEM((steps, block, width // across), f32),
            pltpu.SemaphoreType.DMA((steps,)),
        ],
        input_output_aliases={} if first else {4: 0},
        compiler_params=params(0, 32),
        cost_estimate=cost(4 * tokens * count * width, 4 * count * width),
        name="weight",
    )(*operands)


def swap(x, axis, mask, size):
    return lax.ppermute(x, axis, [(i, i ^ mask) for i in range(size)])


def split(total, unit):
    tiles = total // unit
    sizes = [1, (tiles - 2) // 2, (tiles - 3) // 2, 2]
    starts = [sum(sizes[:i]) for i in range(len(sizes))]
    return [(a * unit, c * unit) for a, c in zip(starts, sizes)]


def thirds(total, unit):
    tiles = total // unit
    sizes = [tiles // 3, tiles - tiles // 3 - tiles // 4, tiles // 4]
    starts = [sum(sizes[:i]) for i in range(3)]
    return [(a * unit, c * unit) for a, c in zip(starts, sizes)]


def fast(n, trunk, branch, unembed, targets, loss_grad):
    block_rows, width = unembed.shape
    seq_index = lax.axis_index("seq")
    ids = jnp.stack([seq_index, lax.axis_index("head"), seq_index * block_rows]).astype(jnp.int32)
    hidden = (trunk.astype(f32) + branch[0].astype(f32)).astype(bf16)
    far = [2, 6, 4]

    pieces = [None] * n
    pieces[0] = hidden
    for k in far:
        pieces[k] = swap(hidden, "seq", k, n)
    for k in [0] + far:
        pieces[k + 1] = swap(pieces[k], "seq", 1, n)

    chunks = split(block_rows, 256)
    late = chunks[2][0]
    staged = []
    for start, count in ((0, late), (late, block_rows - late)):
        staged.append(stage_call(ids, unembed, start, count))
    scores = []
    for c, (start, count) in enumerate(chunks):
        if c == 0:
            s, all_hidden, turned = first_call(ids, pieces, staged[0], count)
        else:
            s = next_call(turned, staged[c // 2], start - c // 2 * late, count)
        s = s.astype(f16)
        scores.append(s.astype(f32) + swap(s, "mp", 1, 2).astype(f32))
    other_hidden = swap(all_hidden, "head", 1, 2)
    so_far, qs = [], []
    for c, (start, count) in enumerate(chunks):
        q, *so_far = numer_call(start, ids, scores[c], targets, so_far)
        qs.append(q)
    half = width // 2
    sums = []
    for r, group in enumerate((qs[:2], qs[2:])):
        for p in range(2):
            sums.append(rows_call(group, staged[r], p * half, half, 512))
    total, stats = so_far
    for i in range(n.bit_length() - 1):
        total = total + swap(total, "seq", 1 << i, n)

    groups = ((4, 6), (2, 0))
    blocks = norm_call(n, groups, ids, total, stats, loss_grad, sums)
    keep, send = blocks[: n // 2], blocks[n // 2 :]
    rows = hidden.shape[0]
    got = []
    for i, group in enumerate(groups):
        theirs = swap(send[i], "seq", 1, n)
        for j, k in enumerate(group):
            both = keep[k // 2] + theirs[j * rows : (j + 1) * rows].astype(f32)
            if k:
                both = swap(both.astype(bf16), "seq", k, n).astype(f32)
            got.append(both)
    row_grad = functools.reduce(lambda a, b: a + b, got)

    g = grads_call(ids, scores, targets, total, loss_grad)
    g_other = swap(g, "head", 1, 2)
    d_unembed, hs = None, [all_hidden, other_hidden]
    for p, (start, count) in enumerate(thirds(block_rows, 256)):
        out = weight_call(ids, g, g_other, hs, start, count, 256, d_unembed)
        d_unembed = out[0]
        if p == 0:
            hs = out[1:]

    d_trunk = row_grad + swap(row_grad, "head", 1, 2)
    return (row_grad.astype(bf16)[None], d_trunk.astype(bf16), d_unembed)


def general(trunk, branch, unembed, targets, loss_grad):
    block_rows = unembed.shape[0]
    hidden = (trunk.astype(f32) + branch[0].astype(f32)).astype(bf16)
    gathered = lax.all_gather(hidden, "seq", axis=0, tiled=True)
    seq_index = lax.axis_index("seq")
    scores = lax.psum(
        lax.dot_general(unembed, gathered, (((1,), (1,)), ((), ())), preferred_element_type=f32),
        "mp",
    )
    exponent, slope = soften(scores)
    totals = lax.psum(jnp.sum(exponent, axis=0), "seq")
    vocab_ids = seq_index * block_rows + lax.iota(jnp.int32, block_rows)
    onehot = (vocab_ids[:, None] == targets[0][None, :]).astype(f32)
    grad_logits = (
        loss_grad[0][None, :] * (exponent / totals[None, :] - onehot) * slope
    ).astype(bf16)
    row_grad = lax.psum_scatter(
        lax.dot_general(grad_logits, unembed, (((0,), (0,)), ((), ())), preferred_element_type=f32),
        "seq",
        scatter_dimension=0,
        tiled=True,
    )
    weight_grad = jnp.dot(grad_logits, gathered, preferred_element_type=f32)
    trunk_sum, unembed_sum = lax.psum((row_grad, weight_grad), "head")
    return (row_grad.astype(bf16)[None], trunk_sum.astype(bf16), unembed_sum)


def solution(mesh):
    in_specs = (
        P("seq", "mp"),
        P("head", "seq", "mp"),
        P("seq", "mp"),
        P("head", None),
        P("head", None),
    )
    out_specs = (P("head", "seq", "mp"), P("seq", "mp"), P("seq", "mp"))
    n = mesh.shape["seq"]
    if mesh.shape["head"] == 2 and mesh.shape["mp"] == 2 and n == 8:

        def body(*args):
            return fast(n, *args)
    else:
        body = general
    step = jax.shard_map(body, mesh=mesh, in_specs=in_specs, out_specs=out_specs, check_vma=False)
    if body is general:
        return step
    return step
```

```python
import functools

import jax
import jax.numpy as jnp
from jax import lax
from jax.experimental import pallas as pl
from jax.experimental.pallas import tpu as pltpu
from jax.sharding import PartitionSpec as P


soft_cap = 30.0
bf16 = jnp.bfloat16
f32 = jnp.float32
f16 = jnp.float16
MIB = 2**20
STAGE_LIMIT = 42


def params(n, limit=12):
    return pltpu.CompilerParams(
        dimension_semantics=("arbitrary",) * n if n else None, vmem_limit_bytes=limit * MIB
    )


def cost(flops, nbytes):
    return pl.CostEstimate(flops=int(flops), bytes_accessed=int(nbytes), transcendentals=0)


def smem():
    return pl.BlockSpec(memory_space=pltpu.SMEM)


def vmem():
    return pl.BlockSpec(memory_space=pltpu.VMEM)


def owner(me, k, n):
    half = n // 2
    return (((me >> 1) + k // 2) & (half - 1)) * 2 + ((me ^ k) & 1)


def stage_kernel(start, ids_ref, u_ref, o_ref, sem):
    copy = pltpu.make_async_copy(u_ref.at[pl.ds(start, o_ref.shape[0])], o_ref, sem)
    copy.start()
    copy.wait()


def stage_call(ids, unembed, start, count):
    shape = (count, unembed.shape[1])
    return pl.pallas_call(
        functools.partial(stage_kernel, start),
        in_specs=[smem(), pl.BlockSpec(memory_space=pltpu.HBM)],
        out_specs=vmem(),
        out_shape=jax.ShapeDtypeStruct(shape, unembed.dtype),
        scratch_shapes=[pltpu.SemaphoreType.DMA],
        compiler_params=params(0, STAGE_LIMIT),
        cost_estimate=cost(count * shape[1], 4 * count * shape[1]),
        name="stage",
    )(ids, unembed)


def first_kernel(n, ids_ref, *refs):
    parts, (u_ref, o_ref, h_ref, ht_ref) = refs[:n], refs[n:]
    rows = parts[0].shape[0]
    for k in range(n):
        at = pl.multiple_of(owner(ids_ref[0], k, n) * rows, rows)
        h_ref[pl.ds(at, rows), :] = parts[k][...]
    ht_ref[...] = h_ref[...].T
    u = u_ref[: o_ref.shape[1], :]
    o_ref[...] = jnp.dot(u, ht_ref[...], preferred_element_type=f32).T


def next_kernel(start, ht_ref, u_ref, o_ref):
    u = u_ref[start : start + o_ref.shape[1], :]
    o_ref[...] = jnp.dot(u, ht_ref[...], preferred_element_type=f32).T


def first_call(ids, pieces, unembed, count):
    width = unembed.shape[1]
    tokens = sum(p.shape[0] for p in pieces)
    return pl.pallas_call(
        functools.partial(first_kernel, len(pieces)),
        in_specs=[smem()] + [vmem()] * (len(pieces) + 1),
        out_specs=[vmem()] * 3,
        out_shape=[
            jax.ShapeDtypeStruct((tokens, count), f32),
            jax.ShapeDtypeStruct((tokens, width), bf16),
            jax.ShapeDtypeStruct((width, tokens), bf16),
        ],
        compiler_params=params(0),
        cost_estimate=cost(2 * tokens * count * width, 2 * count * width),
        name="scores_first",
    )(ids, *pieces, unembed)


def next_call(turned, unembed, start, count):
    width, tokens = turned.shape
    return pl.pallas_call(
        functools.partial(next_kernel, start),
        in_specs=[vmem()] * 2,
        out_specs=vmem(),
        out_shape=jax.ShapeDtypeStruct((tokens, count), f32),
        compiler_params=params(0),
        cost_estimate=cost(2 * tokens * count * width, 2 * count * width),
        name="scores_next",
    )(turned, unembed)


def soften(s):
    squashed = jnp.tanh(s * (1.0 / soft_cap))
    return jnp.exp(soft_cap * squashed), 1.0 - squashed * squashed


def hits(first, targets, shape):
    ids = first + lax.broadcasted_iota(jnp.int32, shape, 1)
    return ids == targets


def column(row):
    return jnp.broadcast_to(row, (row.shape[1], row.shape[1])).T[:, :1]


def numer_kernel(start, first, last, ids_ref, s_ref, *refs):
    tokens, rows = s_ref.shape
    lane = 128
    if first:
        t_ref, refs = refs[0], refs[1:]
        targets = jnp.broadcast_to(column(t_ref[...]), (tokens, lane))
        sums = [jnp.zeros((tokens, lane), f32)] * 3
    else:
        spread_ref, so_far_ref, refs = refs[0], refs[1], refs[2:]
        targets = spread_ref[...]
        sums = [so_far_ref[k] for k in range(3)]
    q_ref, refs = refs[0], refs[1:]
    for j in range(0, rows, lane):
        e, d = soften(s_ref[:, j : j + lane])
        hit = hits(ids_ref[2] + (start + j), targets, e.shape)
        q = e * d
        q_ref[:tokens, j : j + lane] = jnp.where(hit, 0.0, q).astype(bf16)
        q_ref[tokens:, j : j + lane] = jnp.where(hit, 1.0, 0.0).astype(bf16)
        sums[0] = sums[0] + e
        sums[1] = sums[1] + jnp.where(hit, q, 0.0)
        sums[2] = sums[2] + jnp.where(hit, d, 0.0)
    if last:
        tot_ref, stat_ref = refs
        tot, sq, sd = (jnp.sum(a.T, axis=0, keepdims=True) for a in sums)
        tot_ref[...] = tot
        stat_ref[:1, :] = sq
        stat_ref[1:2, :] = sd
    else:
        if first:
            refs[1][...] = targets
        for k in range(3):
            refs[0][k] = sums[k]


def numer_call(start, first, last, ids, s, operands):
    tokens, rows = s.shape
    out_shape = [jax.ShapeDtypeStruct((2 * tokens, rows), bf16)]
    if last:
        out_shape.append(jax.ShapeDtypeStruct((1, tokens), f32))
        out_shape.append(jax.ShapeDtypeStruct((2, tokens), f32))
    else:
        out_shape.append(jax.ShapeDtypeStruct((3, tokens, 128), f32))
    if first:
        out_shape.append(jax.ShapeDtypeStruct((tokens, 128), jnp.int32))
    return pl.pallas_call(
        functools.partial(numer_kernel, start, first, last),
        in_specs=[smem()] + [vmem()] * (1 + len(operands)),
        out_specs=[vmem()] * len(out_shape),
        out_shape=out_shape,
        compiler_params=params(0),
        cost_estimate=cost(40 * tokens * rows, 8 * tokens * rows),
        name="numer",
    )(ids, s, *operands)


def rows_kernel(block, first, places, *refs):
    q_refs, u_refs, o_ref = refs[: len(places)], refs[len(places) : -1], refs[-1]
    step = pl.program_id(0) * block
    cols = pl.ds(pl.multiple_of(first + step, block), block)
    total = None
    for q_ref, (which, row) in zip(q_refs, places):
        u = u_refs[which][row : row + q_ref.shape[1], cols]
        part = jnp.dot(q_ref[...], u, preferred_element_type=f32)
        total = part if total is None else total + part
    o_ref[...] = total


def rows_call(qs, staged, places, first, width, block):
    two = qs[0].shape[0]
    rows = sum(q.shape[1] for q in qs)
    return pl.pallas_call(
        functools.partial(rows_kernel, block, first, places),
        grid=(width // block,),
        in_specs=[vmem()] * (len(qs) + len(staged)),
        out_specs=pl.BlockSpec((two, block), lambda i: (0, i)),
        out_shape=jax.ShapeDtypeStruct((two, width), f32),
        compiler_params=params(1),
        cost_estimate=cost(2 * two * rows * width, 2 * rows * width),
        name="rows",
    )(*qs, *staged)


def norm_kernel(n, groups, parts, ids_ref, tot_ref, stat_ref, lg_ref, *refs):
    sums, refs = refs[:parts], refs[parts:]
    keep, send = refs[: n // 2], refs[n // 2 : n // 2 + len(groups)]
    sc, wc = refs[-2:]
    tokens = tot_ref.shape[1]
    rows = tokens // n
    total = tot_ref[...]
    lg = lg_ref[...]
    sc[...] = jnp.broadcast_to(lg / total, (tokens, tokens)).T
    weight = lg * (stat_ref[:1, :] / total - stat_ref[1:2, :])
    wc[...] = jnp.broadcast_to(weight, (tokens, tokens)).T

    def block(k, ref, row):
        at = pl.multiple_of(owner(ids_ref[0], k, n) * rows, rows)
        scale = sc[pl.ds(at, rows), :1]
        weight = wc[pl.ds(at, rows), :1]
        col = 0
        for x in sums:
            cols = slice(col, col + x.shape[1])
            a = x[pl.ds(at, rows), :]
            u = x[pl.ds(tokens + at, rows), :]
            ref[row : row + rows, cols] = (scale * a + weight * u).astype(ref.dtype)
            col += x.shape[1]

    for ref, group in zip(send, groups):
        for i, k in enumerate(group):
            block(k + 1, ref, i * rows)
    for k in range(0, n, 2):
        block(k, keep[k // 2], 0)


def norm_call(n, groups, ids, total, stats, loss_grad, sums):
    tokens = total.shape[1]
    width = sum(x.shape[1] for x in sums)
    rows = tokens // n
    return pl.pallas_call(
        functools.partial(norm_kernel, n, groups, len(sums)),
        in_specs=[smem()] + [vmem()] * (3 + len(sums)),
        out_specs=[vmem()] * (n // 2 + len(groups)),
        out_shape=[jax.ShapeDtypeStruct((rows, width), f32)] * (n // 2)
        + [jax.ShapeDtypeStruct((rows * len(g), width), bf16) for g in groups],
        scratch_shapes=[pltpu.VMEM((tokens, tokens), f32)] * 2,
        compiler_params=params(0),
        cost_estimate=cost(4 * tokens * width, 10 * tokens * width),
        name="norm",
    )(ids, total, stats, loss_grad, *sums)


def grads_kernel(count, ids_ref, t_ref, tot_ref, lg_ref, *refs):
    g_ref = refs[count]
    inv = column(1.0 / tot_ref[...])
    lg = column(lg_ref[...])
    targets = t_ref[...]
    step = 128
    at = 0
    for s_ref in refs[:count]:
        for j in range(0, s_ref.shape[1], step):
            e, d = soften(s_ref[:, j : j + step])
            hit = hits(ids_ref[2] + at, targets, e.shape)
            p = jnp.where(hit, e * inv - 1.0, e * inv)
            g_ref[:, at : at + step] = (lg * p * d).astype(bf16)
            at += step


def grads_call(ids, scores, targets, total, loss_grad):
    tokens = total.shape[1]
    rows = sum(s.shape[1] for s in scores)
    return pl.pallas_call(
        functools.partial(grads_kernel, len(scores)),
        in_specs=[smem()] + [vmem()] * (3 + len(scores)),
        out_specs=vmem(),
        out_shape=jax.ShapeDtypeStruct((tokens, rows), bf16),
        compiler_params=params(0),
        cost_estimate=cost(40 * tokens * rows, 6 * tokens * rows),
        name="grads",
    )(ids, targets, total, loss_grad, *scores)


def weight_kernel(first, start, block, ids_ref, *refs):
    g0_ref, g1_ref, refs = refs[0], refs[1], refs[2:]
    if first:
        h0_ref, h1_ref, o_ref, h_ref, g_ref, r_ref, sem = refs
    else:
        h_ref, _, o_ref, g_ref, r_ref, sem = refs
    tokens, count = g0_ref.shape[0], g_ref.shape[1]
    mine = pl.multiple_of(ids_ref[1] * tokens, tokens)
    other = pl.multiple_of((1 - ids_ref[1]) * tokens, tokens)
    if first:
        h_ref[pl.ds(mine, tokens), :] = h0_ref[...]
        h_ref[pl.ds(other, tokens), :] = h1_ref[...]
    g_ref[pl.ds(mine, tokens), :] = g0_ref[:, start : start + count]
    g_ref[pl.ds(other, tokens), :] = g1_ref[:, start : start + count]
    turned = g_ref[...].T
    copies = []
    part = r_ref.shape[2]
    across = h_ref.shape[1] // part
    for i in range(r_ref.shape[0]):
        row, col = i // across * block, i % across * part
        r_ref[i] = jnp.dot(
            turned[row : row + block, :],
            h_ref[:, col : col + part],
            preferred_element_type=f32,
        )
        copies.append(
            pltpu.make_async_copy(
                r_ref.at[i],
                o_ref.at[pl.ds(start + row, block), pl.ds(col, part)],
                sem.at[i],
            )
        )
        copies[-1].start()
    for copy in copies:
        copy.wait()


def weight_call(ids, g0, g1, hs, start, count, block, into):
    tokens, rows = g0.shape
    width = hs[0].shape[1]
    hbm = pl.BlockSpec(memory_space=pltpu.HBM)
    first = into is None
    operands = [ids, g0, g1, *hs] + ([] if first else [into])
    specs = [smem()] + [vmem()] * (2 + len(hs)) + ([] if first else [hbm])
    out_specs = [hbm] + ([vmem()] if first else [])
    out_shape = [jax.ShapeDtypeStruct((rows, width), f32)]
    if first:
        out_shape.append(jax.ShapeDtypeStruct((2 * tokens, width), bf16))
    across = 4
    steps = count // block * across
    return pl.pallas_call(
        functools.partial(weight_kernel, first, start, block),
        in_specs=specs,
        out_specs=out_specs,
        out_shape=out_shape,
        scratch_shapes=[
            pltpu.VMEM((2 * tokens, count), bf16),
            pltpu.VMEM((steps, block, width // across), f32),
            pltpu.SemaphoreType.DMA((steps,)),
        ],
        input_output_aliases={} if first else {4: 0},
        compiler_params=params(0, 32),
        cost_estimate=cost(4 * tokens * count * width, 4 * count * width),
        name="weight",
    )(*operands)


def slide(x, by, n):
    half = n // 2
    return lax.ppermute(x, "seq", [(i, (i // 2 + by) % half * 2 + i % 2) for i in range(n)])


def swap(x, axis, mask, size):
    return lax.ppermute(x, axis, [(i, i ^ mask) for i in range(size)])


def split(total, unit):
    tiles = total // unit
    sizes = [1, (tiles - 2) // 2, (tiles - 3) // 2, 2]
    starts = [sum(sizes[:i]) for i in range(len(sizes))]
    return [(a * unit, c * unit) for a, c in zip(starts, sizes)]


def portions(total, unit):
    tiles = total // unit
    sizes = [tiles - tiles // 3 - 2, 1, tiles // 3, 1]
    starts = [sum(sizes[:i]) for i in range(len(sizes))]
    return [(a * unit, c * unit) for a, c in zip(starts, sizes)]


def sides(total, unit):
    tiles = total // unit
    sizes = [(tiles + 1) // 3, tiles // 4, tiles - (tiles + 1) // 3 - tiles // 4]
    starts = [sum(sizes[:i]) for i in range(len(sizes))]
    return [(a * unit, c * unit) for a, c in zip(starts, sizes)]


def fast(n, trunk, branch, unembed, targets, loss_grad):
    block_rows, width = unembed.shape
    seq_index = lax.axis_index("seq")
    ids = jnp.stack([seq_index, lax.axis_index("head"), seq_index * block_rows]).astype(jnp.int32)
    hidden = (trunk.astype(f32) + branch[0].astype(f32)).astype(bf16)
    far = [2 * (i + 1) for i in range(n // 2 - 1)]
    far = far[:1] + far[1:][::-1]

    pieces = [None] * n
    pieces[0] = hidden
    for k in far:
        pieces[k] = slide(hidden, -k // 2, n)
    for k in [0] + far:
        pieces[k + 1] = swap(pieces[k], "seq", 1, n)

    chunks = split(block_rows, 256)
    late = chunks[2][0]
    staged = []
    for start, count in ((0, late), *chunks[2:]):
        staged.append(stage_call(ids, unembed, start, count))
    places = ((0, 0), (0, chunks[1][0]), (1, 0), (2, 0))
    scores = []
    for c, (start, count) in enumerate(chunks):
        if c == 0:
            s, all_hidden, turned = first_call(ids, pieces, staged[0], count)
        else:
            s = next_call(turned, staged[places[c][0]], places[c][1], count)
        s = s.astype(f16)
        scores.append(s.astype(f32) + swap(s, "mp", 1, 2).astype(f32))
    other_hidden = swap(all_hidden, "head", 1, 2)
    qs, spread, so_far = [], None, None
    for c, (start, count) in enumerate(chunks):
        last = c == len(chunks) - 1
        operands = [spread, so_far] if c else [targets]
        q, *out = numer_call(start, c == 0, last, ids, scores[c], operands)
        qs.append(q)
        if c == 0:
            so_far, spread = out
        elif not last:
            so_far = out[0]
    total, stats = out
    sums = []
    for start, count in sides(width, 512):
        sums.append(rows_call(qs, staged, places, start, count, 512))
    for i in range(n.bit_length() - 1):
        total = total + swap(total, "seq", 1 << i, n)

    groups = ((4, 2), (6, 0))
    blocks = norm_call(n, groups, ids, total, stats, loss_grad, sums)
    keep, send = blocks[: n // 2], blocks[n // 2 :]
    rows = hidden.shape[0]
    got = []
    for i, group in enumerate(groups):
        theirs = swap(send[i], "seq", 1, n)
        for j, k in enumerate(group):
            both = keep[k // 2] + theirs[j * rows : (j + 1) * rows].astype(f32)
            if k:
                both = slide(both.astype(bf16), k // 2, n).astype(f32)
            got.append(both)
    row_grad = functools.reduce(lambda a, b: a + b, got)

    g = grads_call(ids, scores, spread, total, loss_grad)
    g_other = swap(g, "head", 1, 2)
    d_unembed, hs = None, [all_hidden, other_hidden]
    for p, (start, count) in enumerate(portions(block_rows, 256)):
        out = weight_call(ids, g, g_other, hs, start, count, 256, d_unembed)
        d_unembed = out[0]
        if p == 0:
            hs = out[1:]

    d_trunk = row_grad + swap(row_grad, "head", 1, 2)
    return (row_grad.astype(bf16)[None], d_trunk.astype(bf16), d_unembed)


def general(trunk, branch, unembed, targets, loss_grad):
    block_rows = unembed.shape[0]
    hidden = (trunk.astype(f32) + branch[0].astype(f32)).astype(bf16)
    gathered = lax.all_gather(hidden, "seq", axis=0, tiled=True)
    seq_index = lax.axis_index("seq")
    scores = lax.psum(
        lax.dot_general(unembed, gathered, (((1,), (1,)), ((), ())), preferred_element_type=f32),
        "mp",
    )
    exponent, slope = soften(scores)
    totals = lax.psum(jnp.sum(exponent, axis=0), "seq")
    vocab_ids = seq_index * block_rows + lax.iota(jnp.int32, block_rows)
    onehot = (vocab_ids[:, None] == targets[0][None, :]).astype(f32)
    grad_logits = (
        loss_grad[0][None, :] * (exponent / totals[None, :] - onehot) * slope
    ).astype(bf16)
    row_grad = lax.psum_scatter(
        lax.dot_general(grad_logits, unembed, (((0,), (0,)), ((), ())), preferred_element_type=f32),
        "seq",
        scatter_dimension=0,
        tiled=True,
    )
    weight_grad = jnp.dot(grad_logits, gathered, preferred_element_type=f32)
    trunk_sum, unembed_sum = lax.psum((row_grad, weight_grad), "head")
    return (row_grad.astype(bf16)[None], trunk_sum.astype(bf16), unembed_sum)


def solution(mesh):
    in_specs = (
        P("seq", "mp"),
        P("head", "seq", "mp"),
        P("seq", "mp"),
        P("head", None),
        P("head", None),
    )
    out_specs = (P("head", "seq", "mp"), P("seq", "mp"), P("seq", "mp"))
    n = mesh.shape["seq"]
    if mesh.shape["head"] == 2 and mesh.shape["mp"] == 2 and n == 8:

        def body(*args):
            return fast(n, *args)
    else:
        body = general
    step = jax.shard_map(body, mesh=mesh, in_specs=in_specs, out_specs=out_specs, check_vma=False)
    if body is general:
        return step
    return step
```

```python
import functools

import jax
import jax.numpy as jnp
from jax import lax
from jax.experimental import pallas as pl
from jax.experimental.pallas import tpu as pltpu
from jax.sharding import PartitionSpec as P


soft_cap = 30.0
bf16 = jnp.bfloat16
f32 = jnp.float32
f16 = jnp.float16
MIB = 2**20


def params(n, limit=12):
    return pltpu.CompilerParams(
        dimension_semantics=("arbitrary",) * n if n else None, vmem_limit_bytes=limit * MIB
    )


def cost(flops, nbytes):
    return pl.CostEstimate(flops=int(flops), bytes_accessed=int(nbytes), transcendentals=0)


def smem():
    return pl.BlockSpec(memory_space=pltpu.SMEM)


def vmem():
    return pl.BlockSpec(memory_space=pltpu.VMEM)


def owner(me, k, n):
    half = n // 2
    return (((me >> 1) + k // 2) & (half - 1)) * 2 + ((me ^ k) & 1)


def tick_kernel(ids_ref, o_ref):
    for k in range(ids_ref.shape[0]):
        o_ref[k] = ids_ref[k]


def tick_call(ids, nbytes):
    return pl.pallas_call(
        tick_kernel,
        in_specs=[smem()],
        out_specs=smem(),
        out_shape=jax.ShapeDtypeStruct(ids.shape, ids.dtype),
        compiler_params=params(0),
        cost_estimate=cost(1000 * nbytes, nbytes),
        name="tick",
    )(ids)


def part_kernel(start, *refs):
    parts, (u_ref, o_ref, h_ref) = refs[:-3], refs[-3:]
    at = 0
    for part in parts:
        h_ref[at : at + part.shape[0], :] = part[...]
        at += part.shape[0]
    u = u_ref[start : start + o_ref.shape[1], :]
    o_ref[...] = jnp.dot(u, h_ref[...].T, preferred_element_type=f32).T


def part_call(pieces, unembed, start, count):
    width = unembed.shape[1]
    tokens = sum(p.shape[0] for p in pieces)
    return pl.pallas_call(
        functools.partial(part_kernel, start),
        in_specs=[vmem()] * (len(pieces) + 1),
        out_specs=vmem(),
        out_shape=jax.ShapeDtypeStruct((tokens, count), f32),
        scratch_shapes=[pltpu.VMEM((tokens, width), bf16)],
        compiler_params=params(0),
        cost_estimate=cost(2 * tokens * count * width, 2 * count * width),
        name="scores_part",
    )(*pieces, unembed)


def first_kernel(n, start, ids_ref, *refs):
    parts, (u_ref, o_ref, h_ref, ht_ref) = refs[:n], refs[n:]
    rows = parts[0].shape[0]
    for k in range(n):
        at = pl.multiple_of(owner(ids_ref[0], k, n) * rows, rows)
        h_ref[pl.ds(at, rows), :] = parts[k][...]
    ht_ref[...] = h_ref[...].T
    u = u_ref[start : start + o_ref.shape[1], :]
    o_ref[...] = jnp.dot(u, ht_ref[...], preferred_element_type=f32).T


def next_kernel(start, ht_ref, u_ref, o_ref):
    u = u_ref[start : start + o_ref.shape[1], :]
    o_ref[...] = jnp.dot(u, ht_ref[...], preferred_element_type=f32).T


def first_call(ids, pieces, unembed, start, count):
    width = unembed.shape[1]
    tokens = sum(p.shape[0] for p in pieces)
    return pl.pallas_call(
        functools.partial(first_kernel, len(pieces), start),
        in_specs=[smem()] + [vmem()] * (len(pieces) + 1),
        out_specs=[vmem()] * 3,
        out_shape=[
            jax.ShapeDtypeStruct((tokens, count), f32),
            jax.ShapeDtypeStruct((tokens, width), bf16),
            jax.ShapeDtypeStruct((width, tokens), bf16),
        ],
        compiler_params=params(0),
        cost_estimate=cost(2 * tokens * count * width, 2 * count * width),
        name="scores_first",
    )(ids, *pieces, unembed)


def next_call(turned, unembed, start, count):
    width, tokens = turned.shape
    return pl.pallas_call(
        functools.partial(next_kernel, start),
        in_specs=[vmem()] * 2,
        out_specs=vmem(),
        out_shape=jax.ShapeDtypeStruct((tokens, count), f32),
        compiler_params=params(0),
        cost_estimate=cost(2 * tokens * count * width, 2 * count * width),
        name="scores_next",
    )(turned, unembed)


def soften(s):
    squashed = jnp.tanh(s * (1.0 / soft_cap))
    return jnp.exp(soft_cap * squashed), 1.0 - squashed * squashed


def hits(first, targets, shape):
    ids = first + lax.broadcasted_iota(jnp.int32, shape, 1)
    return ids == targets


def column(row):
    return jnp.broadcast_to(row, (row.shape[1], row.shape[1])).T[:, :1]


def numer_kernel(start, first, last, n, groups, ids_ref, s_ref, *refs):
    lane = 128
    if groups:
        rest_ref, refs, full_ref = refs[0], refs[1:-1], refs[-1]
        for ref, group in zip((s_ref, rest_ref), groups):
            rows = ref.shape[0] // len(group)
            for i, k in enumerate(group):
                at = pl.multiple_of(owner(ids_ref[0], k, n) * rows, rows)
                full_ref[pl.ds(at, rows), :] = ref[i * rows : (i + 1) * rows, :]
        s_ref = full_ref
    tokens, rows = s_ref.shape
    if first:
        t_ref, refs = refs[0], refs[1:]
        targets = jnp.broadcast_to(column(t_ref[...]), (tokens, lane))
        sums = [jnp.zeros((tokens, lane), f32)] * 3
    else:
        spread_ref, so_far_ref, refs = refs[0], refs[1], refs[2:]
        targets = spread_ref[...]
        sums = [so_far_ref[k] for k in range(3)]
    q_ref, refs = refs[0], refs[1:]
    for j in range(0, rows, lane):
        e, d = soften(s_ref[:, j : j + lane])
        hit = hits(ids_ref[2] + (start + j), targets, e.shape)
        q = e * d
        q_ref[:tokens, j : j + lane] = jnp.where(hit, 0.0, q).astype(bf16)
        q_ref[tokens:, j : j + lane] = jnp.where(hit, 1.0, 0.0).astype(bf16)
        sums[0] = sums[0] + e
        sums[1] = sums[1] + jnp.where(hit, q, 0.0)
        sums[2] = sums[2] + jnp.where(hit, d, 0.0)
    if last:
        tot_ref, stat_ref = refs
        tot, sq, sd = (jnp.sum(a.T, axis=0, keepdims=True) for a in sums)
        tot_ref[...] = tot
        stat_ref[:1, :] = sq
        stat_ref[1:2, :] = sd
    else:
        if first:
            refs[1][...] = targets
        for k in range(3):
            refs[0][k] = sums[k]


def numer_call(start, first, last, n, groups, ids, scores, operands):
    tokens, rows = sum(s.shape[0] for s in scores), scores[0].shape[1]
    out_shape = [jax.ShapeDtypeStruct((2 * tokens, rows), bf16)]
    if last:
        out_shape.append(jax.ShapeDtypeStruct((1, tokens), f32))
        out_shape.append(jax.ShapeDtypeStruct((2, tokens), f32))
    else:
        out_shape.append(jax.ShapeDtypeStruct((3, tokens, 128), f32))
    if first:
        out_shape.append(jax.ShapeDtypeStruct((tokens, 128), jnp.int32))
    if groups:
        out_shape.append(jax.ShapeDtypeStruct((tokens, rows), f32))
    return pl.pallas_call(
        functools.partial(numer_kernel, start, first, last, n, groups),
        in_specs=[smem()] + [vmem()] * (len(scores) + len(operands)),
        out_specs=[vmem()] * len(out_shape),
        out_shape=out_shape,
        compiler_params=params(0),
        cost_estimate=cost(40 * tokens * rows, 8 * tokens * rows),
        name="numer",
    )(ids, *scores, *operands)


def rows_kernel(block, first, places, *refs):
    q_refs, u_refs, o_ref = refs[: len(places)], refs[len(places) : -1], refs[-1]
    step = pl.program_id(0) * block
    cols = pl.ds(pl.multiple_of(first + step, block), block)
    total = None
    for q_ref, (which, row) in zip(q_refs, places):
        u = u_refs[which][row : row + q_ref.shape[1], cols]
        part = jnp.dot(q_ref[...], u, preferred_element_type=f32)
        total = part if total is None else total + part
    o_ref[...] = total


def rows_call(qs, staged, places, first, width, block):
    two = qs[0].shape[0]
    rows = sum(q.shape[1] for q in qs)
    return pl.pallas_call(
        functools.partial(rows_kernel, block, first, places),
        grid=(width // block,),
        in_specs=[vmem()] * (len(qs) + len(staged)),
        out_specs=pl.BlockSpec((two, block), lambda i: (0, i)),
        out_shape=jax.ShapeDtypeStruct((two, width), f32),
        compiler_params=params(1),
        cost_estimate=cost(2 * two * rows * width, 2 * rows * width),
        name="rows",
    )(*qs, *staged)


def norm_kernel(n, groups, parts, ids_ref, tot_ref, stat_ref, lg_ref, *refs):
    sums, refs = refs[:parts], refs[parts:]
    keep, send = refs[: n // 2], refs[n // 2 : n // 2 + len(groups)]
    sc, wc = refs[-2:]
    tokens = tot_ref.shape[1]
    rows = tokens // n
    total = tot_ref[...]
    lg = lg_ref[...]
    sc[...] = jnp.broadcast_to(lg / total, (tokens, tokens)).T
    weight = lg * (stat_ref[:1, :] / total - stat_ref[1:2, :])
    wc[...] = jnp.broadcast_to(weight, (tokens, tokens)).T

    def block(k, ref, row):
        at = pl.multiple_of(owner(ids_ref[0], k, n) * rows, rows)
        scale = sc[pl.ds(at, rows), :1]
        weight = wc[pl.ds(at, rows), :1]
        col = 0
        for x in sums:
            cols = slice(col, col + x.shape[1])
            a = x[pl.ds(at, rows), :]
            u = x[pl.ds(tokens + at, rows), :]
            ref[row : row + rows, cols] = (scale * a + weight * u).astype(ref.dtype)
            col += x.shape[1]

    for ref, group in zip(send, groups):
        for i, k in enumerate(group):
            block(k + 1, ref, i * rows)
    for k in range(0, n, 2):
        block(k, keep[k // 2], 0)


def norm_call(n, groups, ids, total, stats, loss_grad, sums):
    tokens = total.shape[1]
    width = sum(x.shape[1] for x in sums)
    rows = tokens // n
    return pl.pallas_call(
        functools.partial(norm_kernel, n, groups, len(sums)),
        in_specs=[smem()] + [vmem()] * (3 + len(sums)),
        out_specs=[vmem()] * (n // 2 + len(groups)),
        out_shape=[jax.ShapeDtypeStruct((rows, width), f32)] * (n // 2)
        + [jax.ShapeDtypeStruct((rows * len(g), width), bf16) for g in groups],
        scratch_shapes=[pltpu.VMEM((tokens, tokens), f32)] * 2,
        compiler_params=params(0),
        cost_estimate=cost(4 * tokens * width, 10 * tokens * width),
        name="norm",
    )(ids, total, stats, loss_grad, *sums)


def grads_kernel(count, ids_ref, t_ref, tot_ref, lg_ref, *refs):
    g_ref = refs[count]
    inv = column(1.0 / tot_ref[...])
    lg = column(lg_ref[...])
    targets = t_ref[...]
    step = 128
    at = 0
    for s_ref in refs[:count]:
        for j in range(0, s_ref.shape[1], step):
            e, d = soften(s_ref[:, j : j + step])
            hit = hits(ids_ref[2] + at, targets, e.shape)
            p = jnp.where(hit, e * inv - 1.0, e * inv)
            g_ref[:, at : at + step] = (lg * p * d).astype(bf16)
            at += step


def grads_call(ids, scores, targets, total, loss_grad):
    tokens = total.shape[1]
    rows = sum(s.shape[1] for s in scores)
    return pl.pallas_call(
        functools.partial(grads_kernel, len(scores)),
        in_specs=[smem()] + [vmem()] * (3 + len(scores)),
        out_specs=vmem(),
        out_shape=jax.ShapeDtypeStruct((tokens, rows), bf16),
        compiler_params=params(0),
        cost_estimate=cost(40 * tokens * rows, 6 * tokens * rows),
        name="grads",
    )(ids, targets, total, loss_grad, *scores)


def weight_kernel(first, start, block, ids_ref, *refs):
    g0_ref, g1_ref, refs = refs[0], refs[1], refs[2:]
    if first:
        h0_ref, h1_ref, o_ref, h_ref, g_ref, r_ref, sem = refs
    else:
        h_ref, _, o_ref, g_ref, r_ref, sem = refs
    tokens, count = g0_ref.shape[0], g_ref.shape[1]
    mine = pl.multiple_of(ids_ref[1] * tokens, tokens)
    other = pl.multiple_of((1 - ids_ref[1]) * tokens, tokens)
    if first:
        h_ref[pl.ds(mine, tokens), :] = h0_ref[...]
        h_ref[pl.ds(other, tokens), :] = h1_ref[...]
    g_ref[pl.ds(mine, tokens), :] = g0_ref[:, start : start + count]
    g_ref[pl.ds(other, tokens), :] = g1_ref[:, start : start + count]
    turned = g_ref[...].T
    copies = []
    part = r_ref.shape[2]
    across = h_ref.shape[1] // part
    for i in range(r_ref.shape[0]):
        row, col = i // across * block, i % across * part
        r_ref[i] = jnp.dot(
            turned[row : row + block, :],
            h_ref[:, col : col + part],
            preferred_element_type=f32,
        )
        copies.append(
            pltpu.make_async_copy(
                r_ref.at[i],
                o_ref.at[pl.ds(start + row, block), pl.ds(col, part)],
                sem.at[i],
            )
        )
        copies[-1].start()
    for copy in copies:
        copy.wait()


def weight_call(ids, g0, g1, hs, start, count, block, into):
    tokens, rows = g0.shape
    width = hs[0].shape[1]
    hbm = pl.BlockSpec(memory_space=pltpu.HBM)
    first = into is None
    operands = [ids, g0, g1, *hs] + ([] if first else [into])
    specs = [smem()] + [vmem()] * (2 + len(hs)) + ([] if first else [hbm])
    out_specs = [hbm] + ([vmem()] if first else [])
    out_shape = [jax.ShapeDtypeStruct((rows, width), f32)]
    if first:
        out_shape.append(jax.ShapeDtypeStruct((2 * tokens, width), bf16))
    across = 4
    steps = count // block * across
    return pl.pallas_call(
        functools.partial(weight_kernel, first, start, block),
        in_specs=specs,
        out_specs=out_specs,
        out_shape=out_shape,
        scratch_shapes=[
            pltpu.VMEM((2 * tokens, count), bf16),
            pltpu.VMEM((steps, block, width // across), f32),
            pltpu.SemaphoreType.DMA((steps,)),
        ],
        input_output_aliases={} if first else {4: 0},
        compiler_params=params(0, 32),
        cost_estimate=cost(4 * tokens * count * width, 4 * count * width),
        name="weight",
    )(*operands)


def slide(x, by, n):
    half = n // 2
    return lax.ppermute(x, "seq", [(i, (i // 2 + by) % half * 2 + i % 2) for i in range(n)])


def swap(x, axis, mask, size):
    return lax.ppermute(x, axis, [(i, i ^ mask) for i in range(size)])


def split(total, unit):
    tiles = total // unit
    sizes = [tiles // 3, (tiles - tiles // 3 - 1) // 2, 0, 1]
    sizes[2] = tiles - sum(sizes)
    starts = [sum(sizes[:i]) for i in range(len(sizes))]
    return [(a * unit, c * unit) for a, c in zip(starts, sizes)]


def portions(total, unit):
    tiles = total // unit
    sizes = [tiles - tiles // 3 - 2, 1, tiles // 3, 1]
    starts = [sum(sizes[:i]) for i in range(len(sizes))]
    return [(a * unit, c * unit) for a, c in zip(starts, sizes)]


def sides(total, unit):
    tiles = total // unit
    sizes = [(tiles + 1) // 3, tiles // 4, tiles - (tiles + 1) // 3 - tiles // 4]
    starts = [sum(sizes[:i]) for i in range(len(sizes))]
    return [(a * unit, c * unit) for a, c in zip(starts, sizes)]


def fast(n, trunk, branch, unembed, targets, loss_grad):
    block_rows, width = unembed.shape
    seq_index = lax.axis_index("seq")
    ids = jnp.stack([seq_index, lax.axis_index("head"), seq_index * block_rows]).astype(jnp.int32)
    hidden = (trunk.astype(f32) + branch[0].astype(f32)).astype(bf16)
    far = [2 * (i + 1) for i in range(n // 2 - 1)]
    far = far[:1] + far[1:][::-1]

    pieces = [None] * n
    pieces[0] = hidden
    for k in far:
        pieces[k] = slide(hidden, -k // 2, n)
    for k in [0] + far:
        pieces[k + 1] = swap(pieces[k], "seq", 1, n)

    chunks = split(block_rows, 256)
    late = chunks[2][0]
    staged = [unembed]
    ids = tick_call(ids, 8 * unembed.size)
    places = tuple((0, start) for start, _ in chunks)

    def exchange(s):
        s = s.astype(f16)
        return s.astype(f32) + swap(s, "mp", 1, 2).astype(f32)

    late = [far[-1] + 1]
    soon = [k for k in range(n) if k not in late]
    order = (0, 1, 2, 3)
    scores = [None] * 4
    part = part_call([pieces[k] for k in soon], unembed, *chunks[0])
    most = exchange(part)
    for c in order[1:]:
        if c == 3:
            part = part_call([pieces[k] for k in late], unembed, *chunks[0])
            rest = exchange(part)
        if c == 1:
            s, all_hidden, turned = first_call(ids, pieces, unembed, *chunks[c])
        else:
            s = next_call(turned, unembed, *chunks[c])
        scores[c] = exchange(s)
    other_hidden = swap(all_hidden, "head", 1, 2)
    qs, spread, so_far = [None] * 4, None, None
    for c in (1, 2, 0, 3):
        first, last = c == 1, c == 3
        operands = [targets] if first else [spread, so_far]
        parts, groups = ([most, rest], (soon, late)) if c == 0 else ([scores[c]], None)
        qs[c], *out = numer_call(
            chunks[c][0], first, last, n, groups, ids, parts, operands
        )
        if c == 0:
            scores[0] = out.pop()
        if first:
            so_far, spread = out
        elif not last:
            so_far = out[0]
    total, stats = out
    sums = []
    for start, count in sides(width, 512):
        sums.append(rows_call(qs, staged, places, start, count, 512))
    for i in range(n.bit_length() - 1):
        total = total + swap(total, "seq", 1 << i, n)

    groups = ((4, 2), (6, 0))
    blocks = norm_call(n, groups, ids, total, stats, loss_grad, sums)
    keep, send = blocks[: n // 2], blocks[n // 2 :]
    rows = hidden.shape[0]
    got = []
    for i, group in enumerate(groups):
        theirs = swap(send[i], "seq", 1, n)
        for j, k in enumerate(group):
            both = keep[k // 2] + theirs[j * rows : (j + 1) * rows].astype(f32)
            if k:
                both = slide(both.astype(bf16), k // 2, n).astype(f32)
            got.append(both)
    row_grad = functools.reduce(lambda a, b: a + b, got)

    g = grads_call(ids, scores, spread, total, loss_grad)
    g_other = swap(g, "head", 1, 2)
    d_unembed, hs = None, [all_hidden, other_hidden]
    for p, (start, count) in enumerate(portions(block_rows, 256)):
        out = weight_call(ids, g, g_other, hs, start, count, 256, d_unembed)
        d_unembed = out[0]
        if p == 0:
            hs = out[1:]

    d_trunk = row_grad + swap(row_grad, "head", 1, 2)
    return (row_grad.astype(bf16)[None], d_trunk.astype(bf16), d_unembed)


def general(trunk, branch, unembed, targets, loss_grad):
    block_rows = unembed.shape[0]
    hidden = (trunk.astype(f32) + branch[0].astype(f32)).astype(bf16)
    gathered = lax.all_gather(hidden, "seq", axis=0, tiled=True)
    seq_index = lax.axis_index("seq")
    scores = lax.psum(
        lax.dot_general(unembed, gathered, (((1,), (1,)), ((), ())), preferred_element_type=f32),
        "mp",
    )
    exponent, slope = soften(scores)
    totals = lax.psum(jnp.sum(exponent, axis=0), "seq")
    vocab_ids = seq_index * block_rows + lax.iota(jnp.int32, block_rows)
    onehot = (vocab_ids[:, None] == targets[0][None, :]).astype(f32)
    grad_logits = (
        loss_grad[0][None, :] * (exponent / totals[None, :] - onehot) * slope
    ).astype(bf16)
    row_grad = lax.psum_scatter(
        lax.dot_general(grad_logits, unembed, (((0,), (0,)), ((), ())), preferred_element_type=f32),
        "seq",
        scatter_dimension=0,
        tiled=True,
    )
    weight_grad = jnp.dot(grad_logits, gathered, preferred_element_type=f32)
    trunk_sum, unembed_sum = lax.psum((row_grad, weight_grad), "head")
    return (row_grad.astype(bf16)[None], trunk_sum.astype(bf16), unembed_sum)


def solution(mesh):
    in_specs = (
        P("seq", "mp"),
        P("head", "seq", "mp"),
        P("seq", "mp"),
        P("head", None),
        P("head", None),
    )
    out_specs = (P("head", "seq", "mp"), P("seq", "mp"), P("seq", "mp"))
    n = mesh.shape["seq"]
    if mesh.shape["head"] == 2 and mesh.shape["mp"] == 2 and n == 8:

        def body(*args):
            return fast(n, *args)
    else:
        body = general
    step = jax.shard_map(body, mesh=mesh, in_specs=in_specs, out_specs=out_specs, check_vma=False)
    if body is general:
        return step
    return step
```

```python
import functools

import jax
import jax.numpy as jnp
from jax import lax
from jax.experimental import pallas as pl
from jax.experimental.pallas import tpu as pltpu
from jax.sharding import PartitionSpec as P


soft_cap = 30.0
bf16 = jnp.bfloat16
f32 = jnp.float32
f16 = jnp.float16
MIB = 2**20


def params(n, limit=12):
    return pltpu.CompilerParams(
        dimension_semantics=("arbitrary",) * n if n else None, vmem_limit_bytes=limit * MIB
    )


def cost(flops, nbytes):
    return pl.CostEstimate(flops=int(flops), bytes_accessed=int(nbytes), transcendentals=0)


def smem():
    return pl.BlockSpec(memory_space=pltpu.SMEM)


def vmem():
    return pl.BlockSpec(memory_space=pltpu.VMEM)


def owner(me, k, n):
    half = n // 2
    return (((me >> 1) + k // 2) & (half - 1)) * 2 + ((me ^ k) & 1)


def tick_kernel(ids_ref, o_ref):
    for k in range(ids_ref.shape[0]):
        o_ref[k] = ids_ref[k]


def tick_call(ids, nbytes):
    return pl.pallas_call(
        tick_kernel,
        in_specs=[smem()],
        out_specs=smem(),
        out_shape=jax.ShapeDtypeStruct(ids.shape, ids.dtype),
        compiler_params=params(0),
        cost_estimate=cost(1000 * nbytes, nbytes),
        name="tick",
    )(ids)


def part_kernel(start, *refs):
    parts, (u_ref, o_ref, h_ref) = refs[:-3], refs[-3:]
    at = 0
    for part in parts:
        h_ref[at : at + part.shape[0], :] = part[...]
        at += part.shape[0]
    u = u_ref[start : start + o_ref.shape[1], :]
    o_ref[...] = jnp.dot(u, h_ref[...].T, preferred_element_type=f32).T


def part_call(pieces, unembed, start, count):
    width = unembed.shape[1]
    tokens = sum(p.shape[0] for p in pieces)
    return pl.pallas_call(
        functools.partial(part_kernel, start),
        in_specs=[vmem()] * (len(pieces) + 1),
        out_specs=vmem(),
        out_shape=jax.ShapeDtypeStruct((tokens, count), f32),
        scratch_shapes=[pltpu.VMEM((tokens, width), bf16)],
        compiler_params=params(0),
        cost_estimate=cost(2 * tokens * count * width, 2 * count * width),
        name="scores_part",
    )(*pieces, unembed)


def first_kernel(n, start, ids_ref, *refs):
    parts, (u_ref, o_ref, h_ref, ht_ref) = refs[:n], refs[n:]
    rows = parts[0].shape[0]
    for k in range(n):
        at = pl.multiple_of(owner(ids_ref[0], k, n) * rows, rows)
        h_ref[pl.ds(at, rows), :] = parts[k][...]
    ht_ref[...] = h_ref[...].T
    u = u_ref[start : start + o_ref.shape[1], :]
    o_ref[...] = jnp.dot(u, ht_ref[...], preferred_element_type=f32).T


def next_kernel(start, ht_ref, u_ref, o_ref):
    u = u_ref[start : start + o_ref.shape[1], :]
    o_ref[...] = jnp.dot(u, ht_ref[...], preferred_element_type=f32).T


def first_call(ids, pieces, unembed, start, count):
    width = unembed.shape[1]
    tokens = sum(p.shape[0] for p in pieces)
    return pl.pallas_call(
        functools.partial(first_kernel, len(pieces), start),
        in_specs=[smem()] + [vmem()] * (len(pieces) + 1),
        out_specs=[vmem()] * 3,
        out_shape=[
            jax.ShapeDtypeStruct((tokens, count), f32),
            jax.ShapeDtypeStruct((tokens, width), bf16),
            jax.ShapeDtypeStruct((width, tokens), bf16),
        ],
        compiler_params=params(0),
        cost_estimate=cost(2 * tokens * count * width, 2 * count * width),
        name="scores_first",
    )(ids, *pieces, unembed)


def next_call(turned, unembed, start, count):
    width, tokens = turned.shape
    return pl.pallas_call(
        functools.partial(next_kernel, start),
        in_specs=[vmem()] * 2,
        out_specs=vmem(),
        out_shape=jax.ShapeDtypeStruct((tokens, count), f32),
        compiler_params=params(0),
        cost_estimate=cost(2 * tokens * count * width, 2 * count * width),
        name="scores_next",
    )(turned, unembed)


def soften(s):
    squashed = jnp.tanh(s * (1.0 / soft_cap))
    return jnp.exp(soft_cap * squashed), 1.0 - squashed * squashed


def hits(first, targets, shape):
    ids = first + lax.broadcasted_iota(jnp.int32, shape, 1)
    return ids == targets


def column(row):
    return jnp.broadcast_to(row, (row.shape[1], row.shape[1])).T[:, :1]


def numer_kernel(start, first, last, n, groups, ids_ref, s_ref, *refs):
    lane = 128
    if groups:
        rest_ref, refs, full_ref = refs[0], refs[1:-1], refs[-1]
        for ref, group in zip((s_ref, rest_ref), groups):
            rows = ref.shape[0] // len(group)
            for i, k in enumerate(group):
                at = pl.multiple_of(owner(ids_ref[0], k, n) * rows, rows)
                full_ref[pl.ds(at, rows), :] = ref[i * rows : (i + 1) * rows, :]
        s_ref = full_ref
    tokens, rows = s_ref.shape
    if first:
        t_ref, refs = refs[0], refs[1:]
        targets = jnp.broadcast_to(column(t_ref[...]), (tokens, lane))
        sums = [jnp.zeros((tokens, lane), f32)] * 3
    else:
        spread_ref, so_far_ref, refs = refs[0], refs[1], refs[2:]
        targets = spread_ref[...]
        sums = [so_far_ref[k] for k in range(3)]
    q_ref, p_ref, refs = refs[0], refs[1], refs[2:]
    for j in range(0, rows, lane):
        e, d = soften(s_ref[:, j : j + lane])
        hit = hits(ids_ref[2] + (start + j), targets, e.shape)
        q = e * d
        p_ref[:, j : j + lane] = q
        q_ref[:tokens, j : j + lane] = jnp.where(hit, 0.0, q).astype(bf16)
        q_ref[tokens:, j : j + lane] = jnp.where(hit, 1.0, 0.0).astype(bf16)
        sums[0] = sums[0] + e
        sums[1] = sums[1] + jnp.where(hit, q, 0.0)
        sums[2] = sums[2] + jnp.where(hit, d, 0.0)
    if last:
        tot_ref, stat_ref = refs
        tot, sq, sd = (jnp.sum(a.T, axis=0, keepdims=True) for a in sums)
        tot_ref[...] = tot
        stat_ref[:1, :] = sq
        stat_ref[1:2, :] = sd
    else:
        if first:
            refs[1][...] = targets
        for k in range(3):
            refs[0][k] = sums[k]


def numer_call(start, first, last, n, groups, ids, scores, operands):
    tokens, rows = sum(s.shape[0] for s in scores), scores[0].shape[1]
    out_shape = [
        jax.ShapeDtypeStruct((2 * tokens, rows), bf16),
        jax.ShapeDtypeStruct((tokens, rows), f32),
    ]
    if last:
        out_shape.append(jax.ShapeDtypeStruct((1, tokens), f32))
        out_shape.append(jax.ShapeDtypeStruct((2, tokens), f32))
    else:
        out_shape.append(jax.ShapeDtypeStruct((3, tokens, 128), f32))
    if first:
        out_shape.append(jax.ShapeDtypeStruct((tokens, 128), jnp.int32))
    return pl.pallas_call(
        functools.partial(numer_kernel, start, first, last, n, groups),
        in_specs=[smem()] + [vmem()] * (len(scores) + len(operands)),
        out_specs=[vmem()] * len(out_shape),
        out_shape=out_shape,
        scratch_shapes=[pltpu.VMEM((tokens, rows), f32)] if groups else [],
        compiler_params=params(0),
        cost_estimate=cost(40 * tokens * rows, 8 * tokens * rows),
        name="numer",
    )(ids, *scores, *operands)


def rows_kernel(block, first, places, *refs):
    q_refs, u_refs, o_ref = refs[: len(places)], refs[len(places) : -1], refs[-1]
    step = pl.program_id(0) * block
    cols = pl.ds(pl.multiple_of(first + step, block), block)
    total = None
    for q_ref, (which, row) in zip(q_refs, places):
        u = u_refs[which][row : row + q_ref.shape[1], cols]
        part = jnp.dot(q_ref[...], u, preferred_element_type=f32)
        total = part if total is None else total + part
    o_ref[...] = total


def rows_call(qs, staged, places, first, width, block):
    two = qs[0].shape[0]
    rows = sum(q.shape[1] for q in qs)
    return pl.pallas_call(
        functools.partial(rows_kernel, block, first, places),
        grid=(width // block,),
        in_specs=[vmem()] * (len(qs) + len(staged)),
        out_specs=pl.BlockSpec((two, block), lambda i: (0, i)),
        out_shape=jax.ShapeDtypeStruct((two, width), f32),
        compiler_params=params(1),
        cost_estimate=cost(2 * two * rows * width, 2 * rows * width),
        name="rows",
    )(*qs, *staged)


def norm_kernel(n, groups, parts, ids_ref, tot_ref, stat_ref, lg_ref, *refs):
    sums, refs = refs[:parts], refs[parts:]
    keep, send = refs[: n // 2], refs[n // 2 : n // 2 + len(groups)]
    sc, wc = refs[-2:]
    tokens = tot_ref.shape[1]
    rows = tokens // n
    total = tot_ref[...]
    lg = lg_ref[...]
    sc[...] = jnp.broadcast_to(lg / total, (tokens, tokens)).T
    weight = lg * (stat_ref[:1, :] / total - stat_ref[1:2, :])
    wc[...] = jnp.broadcast_to(weight, (tokens, tokens)).T

    def block(k, ref, row):
        at = pl.multiple_of(owner(ids_ref[0], k, n) * rows, rows)
        scale = sc[pl.ds(at, rows), :1]
        weight = wc[pl.ds(at, rows), :1]
        col = 0
        for x in sums:
            cols = slice(col, col + x.shape[1])
            a = x[pl.ds(at, rows), :]
            u = x[pl.ds(tokens + at, rows), :]
            ref[row : row + rows, cols] = (scale * a + weight * u).astype(ref.dtype)
            col += x.shape[1]

    for ref, group in zip(send, groups):
        for i, k in enumerate(group):
            block(k + 1, ref, i * rows)
    for k in range(0, n, 2):
        block(k, keep[k // 2], 0)


def norm_call(n, groups, ids, total, stats, loss_grad, sums):
    tokens = total.shape[1]
    width = sum(x.shape[1] for x in sums)
    rows = tokens // n
    return pl.pallas_call(
        functools.partial(norm_kernel, n, groups, len(sums)),
        in_specs=[smem()] + [vmem()] * (3 + len(sums)),
        out_specs=[vmem()] * (n // 2 + len(groups)),
        out_shape=[jax.ShapeDtypeStruct((rows, width), f32)] * (n // 2)
        + [jax.ShapeDtypeStruct((rows * len(g), width), bf16) for g in groups],
        scratch_shapes=[pltpu.VMEM((tokens, tokens), f32)] * 2,
        compiler_params=params(0),
        cost_estimate=cost(4 * tokens * width, 10 * tokens * width),
        name="norm",
    )(ids, total, stats, loss_grad, *sums)


def grads_kernel(ids_ref, t_ref, tot_ref, stat_ref, lg_ref, *refs):
    g_ref = refs[-1]
    scale = column(lg_ref[...] / tot_ref[...])
    peak = column(lg_ref[...] * stat_ref[1:2, :])
    targets = t_ref[...]
    step = 128
    at = 0
    for p_ref in refs[:-1]:
        for j in range(0, p_ref.shape[1], step):
            p = scale * p_ref[:, j : j + step]
            hit = hits(ids_ref[2] + at, targets, p.shape)
            g_ref[:, at : at + step] = jnp.where(hit, p - peak, p).astype(bf16)
            at += step


def grads_call(ids, numers, targets, total, stats, loss_grad):
    tokens = total.shape[1]
    rows = sum(p.shape[1] for p in numers)
    return pl.pallas_call(
        grads_kernel,
        in_specs=[smem()] + [vmem()] * (4 + len(numers)),
        out_specs=vmem(),
        out_shape=jax.ShapeDtypeStruct((tokens, rows), bf16),
        compiler_params=params(0),
        cost_estimate=cost(4 * tokens * rows, 6 * tokens * rows),
        name="grads",
    )(ids, targets, total, stats, loss_grad, *numers)


def weight_kernel(first, start, block, ids_ref, *refs):
    g0_ref, g1_ref, refs = refs[0], refs[1], refs[2:]
    if first:
        h0_ref, h1_ref, o_ref, h_ref, g_ref, r_ref, sem = refs
    else:
        h_ref, _, o_ref, g_ref, r_ref, sem = refs
    tokens, count = g0_ref.shape[0], g_ref.shape[1]
    mine = pl.multiple_of(ids_ref[1] * tokens, tokens)
    other = pl.multiple_of((1 - ids_ref[1]) * tokens, tokens)
    if first:
        h_ref[pl.ds(mine, tokens), :] = h0_ref[...]
        h_ref[pl.ds(other, tokens), :] = h1_ref[...]
    g_ref[pl.ds(mine, tokens), :] = g0_ref[:, start : start + count]
    g_ref[pl.ds(other, tokens), :] = g1_ref[:, start : start + count]
    turned = g_ref[...].T
    copies = []
    part = r_ref.shape[2]
    across = h_ref.shape[1] // part
    for i in range(r_ref.shape[0]):
        row, col = i // across * block, i % across * part
        r_ref[i] = jnp.dot(
            turned[row : row + block, :],
            h_ref[:, col : col + part],
            preferred_element_type=f32,
        )
        copies.append(
            pltpu.make_async_copy(
                r_ref.at[i],
                o_ref.at[pl.ds(start + row, block), pl.ds(col, part)],
                sem.at[i],
            )
        )
        copies[-1].start()
    for copy in copies:
        copy.wait()


def weight_call(ids, g0, g1, hs, start, count, block, into):
    tokens, rows = g0.shape
    width = hs[0].shape[1]
    hbm = pl.BlockSpec(memory_space=pltpu.HBM)
    first = into is None
    operands = [ids, g0, g1, *hs] + ([] if first else [into])
    specs = [smem()] + [vmem()] * (2 + len(hs)) + ([] if first else [hbm])
    out_specs = [hbm] + ([vmem()] if first else [])
    out_shape = [jax.ShapeDtypeStruct((rows, width), f32)]
    if first:
        out_shape.append(jax.ShapeDtypeStruct((2 * tokens, width), bf16))
    across = 8
    steps = count // block * across
    return pl.pallas_call(
        functools.partial(weight_kernel, first, start, block),
        in_specs=specs,
        out_specs=out_specs,
        out_shape=out_shape,
        scratch_shapes=[
            pltpu.VMEM((2 * tokens, count), bf16),
            pltpu.VMEM((steps, block, width // across), f32),
            pltpu.SemaphoreType.DMA((steps,)),
        ],
        input_output_aliases={} if first else {4: 0},
        compiler_params=params(0, 32),
        cost_estimate=cost(4 * tokens * count * width, 4 * count * width),
        name="weight",
    )(*operands)


def slide(x, by, n):
    half = n // 2
    return lax.ppermute(x, "seq", [(i, (i // 2 + by) % half * 2 + i % 2) for i in range(n)])


def swap(x, axis, mask, size):
    return lax.ppermute(x, axis, [(i, i ^ mask) for i in range(size)])


def split(total, unit):
    tiles = total // unit
    sizes = [tiles // 3, (tiles - tiles // 3 - 1) // 2, 0, 1]
    sizes[2] = tiles - sum(sizes)
    starts = [sum(sizes[:i]) for i in range(len(sizes))]
    return [(a * unit, c * unit) for a, c in zip(starts, sizes)]


def portions(total, unit):
    tiles = total // unit
    sizes = [tiles // 2, tiles - tiles // 2 - 1, 1]
    starts = [sum(sizes[:i]) for i in range(len(sizes))]
    return [(a * unit, c * unit) for a, c in zip(starts, sizes)]


def sides(total, unit):
    tiles = total // unit
    sizes = [(tiles + 1) // 3, tiles // 4, tiles - (tiles + 1) // 3 - tiles // 4]
    starts = [sum(sizes[:i]) for i in range(len(sizes))]
    return [(a * unit, c * unit) for a, c in zip(starts, sizes)]


def fast(n, trunk, branch, unembed, targets, loss_grad):
    block_rows, width = unembed.shape
    seq_index = lax.axis_index("seq")
    ids = jnp.stack([seq_index, lax.axis_index("head"), seq_index * block_rows]).astype(jnp.int32)
    hidden = (trunk.astype(f32) + branch[0].astype(f32)).astype(bf16)
    far = [2 * (i + 1) for i in range(n // 2 - 1)]
    far = far[:1] + far[1:][::-1]

    pieces = [None] * n
    pieces[0] = hidden
    for k in far:
        pieces[k] = slide(hidden, -k // 2, n)
    for k in [0] + far:
        pieces[k + 1] = swap(pieces[k], "seq", 1, n)

    chunks = split(block_rows, 256)
    late = chunks[2][0]
    staged = [unembed]
    ids = tick_call(ids, 8 * unembed.size)
    places = tuple((0, start) for start, _ in chunks)

    def exchange(s):
        s = s.astype(f16)
        return s.astype(f32) + swap(s, "mp", 1, 2).astype(f32)

    late = [far[-1] + 1]
    soon = [k for k in range(n) if k not in late]
    order = (0, 1, 2, 3)
    scores = [None] * 4
    part = part_call([pieces[k] for k in soon], unembed, *chunks[0])
    most = exchange(part)
    for c in order[1:]:
        if c == 3:
            part = part_call([pieces[k] for k in late], unembed, *chunks[0])
            rest = exchange(part)
        if c == 1:
            s, all_hidden, turned = first_call(ids, pieces, unembed, *chunks[c])
        else:
            s = next_call(turned, unembed, *chunks[c])
        scores[c] = exchange(s)
    other_hidden = swap(all_hidden, "head", 1, 2)
    qs, ps, spread, so_far = [None] * 4, [None] * 4, None, None
    for c in (1, 2, 0, 3):
        first, last = c == 1, c == 3
        operands = [targets] if first else [spread, so_far]
        parts, groups = ([most, rest], (soon, late)) if c == 0 else ([scores[c]], None)
        qs[c], ps[c], *out = numer_call(
            chunks[c][0], first, last, n, groups, ids, parts, operands
        )
        if first:
            so_far, spread = out
        elif not last:
            so_far = out[0]
    total, stats = out
    sums = []
    for start, count in sides(width, 512):
        sums.append(rows_call(qs, staged, places, start, count, 512))
    for i in range(n.bit_length() - 1):
        total = total + swap(total, "seq", 1 << i, n)

    groups = ((4, 2), (6, 0))
    blocks = norm_call(n, groups, ids, total, stats, loss_grad, sums)
    keep, send = blocks[: n // 2], blocks[n // 2 :]
    rows = hidden.shape[0]
    got = []
    for i, group in enumerate(groups):
        theirs = swap(send[i], "seq", 1, n)
        for j, k in enumerate(group):
            both = keep[k // 2] + theirs[j * rows : (j + 1) * rows].astype(f32)
            if k:
                both = slide(both.astype(bf16), k // 2, n).astype(f32)
            got.append(both)
    row_grad = functools.reduce(lambda a, b: a + b, got)

    g = grads_call(ids, ps, spread, total, stats, loss_grad)
    g_other = swap(g, "head", 1, 2)
    d_unembed, hs = None, [all_hidden, other_hidden]
    for p, (start, count) in enumerate(portions(block_rows, 128)):
        block = 128 if count % 256 else 256
        out = weight_call(ids, g, g_other, hs, start, count, block, d_unembed)
        d_unembed = out[0]
        if p == 0:
            hs = out[1:]

    d_trunk = row_grad + swap(row_grad, "head", 1, 2)
    return (row_grad.astype(bf16)[None], d_trunk.astype(bf16), d_unembed)


def general(trunk, branch, unembed, targets, loss_grad):
    block_rows = unembed.shape[0]
    hidden = (trunk.astype(f32) + branch[0].astype(f32)).astype(bf16)
    gathered = lax.all_gather(hidden, "seq", axis=0, tiled=True)
    seq_index = lax.axis_index("seq")
    scores = lax.psum(
        lax.dot_general(unembed, gathered, (((1,), (1,)), ((), ())), preferred_element_type=f32),
        "mp",
    )
    exponent, slope = soften(scores)
    totals = lax.psum(jnp.sum(exponent, axis=0), "seq")
    vocab_ids = seq_index * block_rows + lax.iota(jnp.int32, block_rows)
    onehot = (vocab_ids[:, None] == targets[0][None, :]).astype(f32)
    grad_logits = (
        loss_grad[0][None, :] * (exponent / totals[None, :] - onehot) * slope
    ).astype(bf16)
    row_grad = lax.psum_scatter(
        lax.dot_general(grad_logits, unembed, (((0,), (0,)), ((), ())), preferred_element_type=f32),
        "seq",
        scatter_dimension=0,
        tiled=True,
    )
    weight_grad = jnp.dot(grad_logits, gathered, preferred_element_type=f32)
    trunk_sum, unembed_sum = lax.psum((row_grad, weight_grad), "head")
    return (row_grad.astype(bf16)[None], trunk_sum.astype(bf16), unembed_sum)


def solution(mesh):
    in_specs = (
        P("seq", "mp"),
        P("head", "seq", "mp"),
        P("seq", "mp"),
        P("head", None),
        P("head", None),
    )
    out_specs = (P("head", "seq", "mp"), P("seq", "mp"), P("seq", "mp"))
    n = mesh.shape["seq"]
    if mesh.shape["head"] == 2 and mesh.shape["mp"] == 2 and n == 8:

        def body(*args):
            return fast(n, *args)
    else:
        body = general
    step = jax.shard_map(body, mesh=mesh, in_specs=in_specs, out_specs=out_specs, check_vma=False)
    if body is general:
        return step
    return step
```

```python
import functools

import jax
import jax.numpy as jnp
from jax import lax
from jax.experimental import pallas as pl
from jax.experimental.pallas import tpu as pltpu
from jax.sharding import PartitionSpec as P


soft_cap = 30.0
bf16 = jnp.bfloat16
f32 = jnp.float32
f16 = jnp.float16
MIB = 2**20


def params(n, limit=12):
    return pltpu.CompilerParams(
        dimension_semantics=("arbitrary",) * n if n else None, vmem_limit_bytes=limit * MIB
    )


def cost(flops, nbytes):
    return pl.CostEstimate(flops=int(flops), bytes_accessed=int(nbytes), transcendentals=0)


def smem():
    return pl.BlockSpec(memory_space=pltpu.SMEM)


def vmem():
    return pl.BlockSpec(memory_space=pltpu.VMEM)


def owner(me, k, n):
    half = n // 2
    return (((me >> 1) + k // 2) & (half - 1)) * 2 + ((me ^ k) & 1)


def tick_kernel(ids_ref, o_ref):
    for k in range(ids_ref.shape[0]):
        o_ref[k] = ids_ref[k]


def tick_call(ids, nbytes):
    return pl.pallas_call(
        tick_kernel,
        in_specs=[smem()],
        out_specs=smem(),
        out_shape=jax.ShapeDtypeStruct(ids.shape, ids.dtype),
        compiler_params=params(0),
        cost_estimate=cost(1000 * nbytes, nbytes),
        name="tick",
    )(ids)


def part_kernel(start, *refs):
    parts, (u_ref, o_ref, h_ref) = refs[:-3], refs[-3:]
    at = 0
    for part in parts:
        h_ref[at : at + part.shape[0], :] = part[...]
        at += part.shape[0]
    u = u_ref[start : start + o_ref.shape[1], :]
    o_ref[...] = jnp.dot(u, h_ref[...].T, preferred_element_type=f32).T


def part_call(pieces, unembed, start, count):
    width = unembed.shape[1]
    tokens = sum(p.shape[0] for p in pieces)
    return pl.pallas_call(
        functools.partial(part_kernel, start),
        in_specs=[vmem()] * (len(pieces) + 1),
        out_specs=vmem(),
        out_shape=jax.ShapeDtypeStruct((tokens, count), f32),
        scratch_shapes=[pltpu.VMEM((tokens, width), bf16)],
        compiler_params=params(0),
        cost_estimate=cost(2 * tokens * count * width, 2 * count * width),
        name="scores_part",
    )(*pieces, unembed)


def first_kernel(n, start, ids_ref, *refs):
    parts, (u_ref, o_ref, h_ref, ht_ref) = refs[:n], refs[n:]
    rows = parts[0].shape[0]
    for k in range(n):
        at = pl.multiple_of(owner(ids_ref[0], k, n) * rows, rows)
        h_ref[pl.ds(at, rows), :] = parts[k][...]
    ht_ref[...] = h_ref[...].T
    u = u_ref[start : start + o_ref.shape[1], :]
    o_ref[...] = jnp.dot(u, ht_ref[...], preferred_element_type=f32).T


def next_kernel(start, ht_ref, u_ref, o_ref):
    u = u_ref[start : start + o_ref.shape[1], :]
    o_ref[...] = jnp.dot(u, ht_ref[...], preferred_element_type=f32).T


def first_call(ids, pieces, unembed, start, count):
    width = unembed.shape[1]
    tokens = sum(p.shape[0] for p in pieces)
    return pl.pallas_call(
        functools.partial(first_kernel, len(pieces), start),
        in_specs=[smem()] + [vmem()] * (len(pieces) + 1),
        out_specs=[vmem()] * 3,
        out_shape=[
            jax.ShapeDtypeStruct((tokens, count), f32),
            jax.ShapeDtypeStruct((tokens, width), bf16),
            jax.ShapeDtypeStruct((width, tokens), bf16),
        ],
        compiler_params=params(0),
        cost_estimate=cost(2 * tokens * count * width, 2 * count * width),
        name="scores_first",
    )(ids, *pieces, unembed)


def next_call(turned, unembed, start, count):
    width, tokens = turned.shape
    return pl.pallas_call(
        functools.partial(next_kernel, start),
        in_specs=[vmem()] * 2,
        out_specs=vmem(),
        out_shape=jax.ShapeDtypeStruct((tokens, count), f32),
        compiler_params=params(0),
        cost_estimate=cost(2 * tokens * count * width, 2 * count * width),
        name="scores_next",
    )(turned, unembed)


def soften(s):
    squashed = jnp.tanh(s * (1.0 / soft_cap))
    return jnp.exp(soft_cap * squashed), 1.0 - squashed * squashed


def hits(first, targets, shape):
    ids = first + lax.broadcasted_iota(jnp.int32, shape, 1)
    return ids == targets


def column(row):
    return jnp.broadcast_to(row, (row.shape[1], row.shape[1])).T[:, :1]


def numer_kernel(start, first, last, n, groups, ids_ref, s_ref, *refs):
    lane = 128
    if groups:
        rest_ref, refs, full_ref = refs[0], refs[1:-1], refs[-1]
        for ref, group in zip((s_ref, rest_ref), groups):
            rows = ref.shape[0] // len(group)
            for i, k in enumerate(group):
                at = pl.multiple_of(owner(ids_ref[0], k, n) * rows, rows)
                full_ref[pl.ds(at, rows), :] = ref[i * rows : (i + 1) * rows, :]
        s_ref = full_ref
    tokens, rows = s_ref.shape
    if first:
        t_ref, refs = refs[0], refs[1:]
        targets = jnp.broadcast_to(column(t_ref[...]), (tokens, lane))
        sums = [jnp.zeros((tokens, lane), f32)] * 3
    else:
        spread_ref, so_far_ref, refs = refs[0], refs[1], refs[2:]
        targets = spread_ref[...]
        sums = [so_far_ref[k] for k in range(3)]
    q_ref, p_ref, refs = refs[0], refs[1], refs[2:]
    for j in range(0, rows, lane):
        e, d = soften(s_ref[:, j : j + lane])
        hit = hits(ids_ref[2] + (start + j), targets, e.shape)
        q = e * d
        p_ref[:, j : j + lane] = q
        q_ref[:tokens, j : j + lane] = jnp.where(hit, 0.0, q).astype(bf16)
        q_ref[tokens:, j : j + lane] = jnp.where(hit, 1.0, 0.0).astype(bf16)
        sums[0] = sums[0] + e
        sums[1] = sums[1] + jnp.where(hit, q, 0.0)
        sums[2] = sums[2] + jnp.where(hit, d, 0.0)
    if last:
        tot_ref, stat_ref = refs
        tot, sq, sd = (jnp.sum(a.T, axis=0, keepdims=True) for a in sums)
        tot_ref[...] = tot
        stat_ref[:1, :] = sq
        stat_ref[1:2, :] = sd
    else:
        if first:
            refs[1][...] = targets
        for k in range(3):
            refs[0][k] = sums[k]


def numer_call(start, first, last, n, groups, ids, scores, operands):
    tokens, rows = sum(s.shape[0] for s in scores), scores[0].shape[1]
    out_shape = [
        jax.ShapeDtypeStruct((2 * tokens, rows), bf16),
        jax.ShapeDtypeStruct((tokens, rows), f32),
    ]
    if last:
        out_shape.append(jax.ShapeDtypeStruct((1, tokens), f32))
        out_shape.append(jax.ShapeDtypeStruct((2, tokens), f32))
    else:
        out_shape.append(jax.ShapeDtypeStruct((3, tokens, 128), f32))
    if first:
        out_shape.append(jax.ShapeDtypeStruct((tokens, 128), jnp.int32))
    return pl.pallas_call(
        functools.partial(numer_kernel, start, first, last, n, groups),
        in_specs=[smem()] + [vmem()] * (len(scores) + len(operands)),
        out_specs=[vmem()] * len(out_shape),
        out_shape=out_shape,
        scratch_shapes=[pltpu.VMEM((tokens, rows), f32)] if groups else [],
        compiler_params=params(0),
        cost_estimate=cost(40 * tokens * rows, 8 * tokens * rows),
        name="numer",
    )(ids, *scores, *operands)


def rows_kernel(block, first, places, *refs):
    q_refs, u_refs, o_ref = refs[: len(places)], refs[len(places) : -1], refs[-1]
    step = pl.program_id(0) * block
    cols = pl.ds(pl.multiple_of(first + step, block), block)
    total = None
    for q_ref, (which, row) in zip(q_refs, places):
        u = u_refs[which][row : row + q_ref.shape[1], cols]
        part = jnp.dot(q_ref[...], u, preferred_element_type=f32)
        total = part if total is None else total + part
    o_ref[...] = total


def rows_call(qs, staged, places, first, width, block):
    two = qs[0].shape[0]
    rows = sum(q.shape[1] for q in qs)
    return pl.pallas_call(
        functools.partial(rows_kernel, block, first, places),
        grid=(width // block,),
        in_specs=[vmem()] * (len(qs) + len(staged)),
        out_specs=pl.BlockSpec((two, block), lambda i: (0, i)),
        out_shape=jax.ShapeDtypeStruct((two, width), f32),
        compiler_params=params(1),
        cost_estimate=cost(2 * two * rows * width, 2 * rows * width),
        name="rows",
    )(*qs, *staged)


def norm_kernel(n, groups, parts, ids_ref, tot_ref, stat_ref, lg_ref, *refs):
    sums, refs = refs[:parts], refs[parts:]
    keep, send = refs[: n // 2], refs[n // 2 : n // 2 + len(groups)]
    sc, wc = refs[-2:]
    tokens = tot_ref.shape[1]
    rows = tokens // n
    total = tot_ref[...]
    lg = lg_ref[...]
    sc[...] = jnp.broadcast_to(lg / total, (tokens, tokens)).T
    weight = lg * (stat_ref[:1, :] / total - stat_ref[1:2, :])
    wc[...] = jnp.broadcast_to(weight, (tokens, tokens)).T

    def block(k, ref, row):
        at = pl.multiple_of(owner(ids_ref[0], k, n) * rows, rows)
        scale = sc[pl.ds(at, rows), :1]
        weight = wc[pl.ds(at, rows), :1]
        col = 0
        for x in sums:
            cols = slice(col, col + x.shape[1])
            a = x[pl.ds(at, rows), :]
            u = x[pl.ds(tokens + at, rows), :]
            ref[row : row + rows, cols] = (scale * a + weight * u).astype(ref.dtype)
            col += x.shape[1]

    for ref, group in zip(send, groups):
        for i, k in enumerate(group):
            block(k + 1, ref, i * rows)
    for k in range(0, n, 2):
        block(k, keep[k // 2], 0)


def norm_call(n, groups, ids, total, stats, loss_grad, sums):
    tokens = total.shape[1]
    width = sum(x.shape[1] for x in sums)
    rows = tokens // n
    return pl.pallas_call(
        functools.partial(norm_kernel, n, groups, len(sums)),
        in_specs=[smem()] + [vmem()] * (3 + len(sums)),
        out_specs=[vmem()] * (n // 2 + len(groups)),
        out_shape=[jax.ShapeDtypeStruct((rows, width), f32)] * (n // 2)
        + [jax.ShapeDtypeStruct((rows * len(g), width), bf16) for g in groups],
        scratch_shapes=[pltpu.VMEM((tokens, tokens), f32)] * 2,
        compiler_params=params(0),
        cost_estimate=cost(4 * tokens * width, 10 * tokens * width),
        name="norm",
    )(ids, total, stats, loss_grad, *sums)


def grads_kernel(ids_ref, t_ref, tot_ref, stat_ref, lg_ref, *refs):
    g_ref = refs[-1]
    scale = column(lg_ref[...] / tot_ref[...])
    peak = column(lg_ref[...] * stat_ref[1:2, :])
    targets = t_ref[...]
    step = 128
    at = 0
    for p_ref in refs[:-1]:
        for j in range(0, p_ref.shape[1], step):
            p = scale * p_ref[:, j : j + step]
            hit = hits(ids_ref[2] + at, targets, p.shape)
            g_ref[:, at : at + step] = jnp.where(hit, p - peak, p).astype(bf16)
            at += step


def grads_call(ids, numers, targets, total, stats, loss_grad):
    tokens = total.shape[1]
    rows = sum(p.shape[1] for p in numers)
    return pl.pallas_call(
        grads_kernel,
        in_specs=[smem()] + [vmem()] * (4 + len(numers)),
        out_specs=vmem(),
        out_shape=jax.ShapeDtypeStruct((tokens, rows), bf16),
        compiler_params=params(0),
        cost_estimate=cost(4 * tokens * rows, 6 * tokens * rows),
        name="grads",
    )(ids, targets, total, stats, loss_grad, *numers)


def join_kernel(ids_ref, h0_ref, h1_ref, o_ref):
    tokens = h0_ref.shape[0]
    o_ref[pl.ds(pl.multiple_of(ids_ref[1] * tokens, tokens), tokens), :] = h0_ref[...]
    o_ref[pl.ds(pl.multiple_of((1 - ids_ref[1]) * tokens, tokens), tokens), :] = h1_ref[...]


def join_call(ids, h0, h1):
    return pl.pallas_call(
        join_kernel,
        in_specs=[smem()] + [vmem()] * 2,
        out_specs=vmem(),
        out_shape=jax.ShapeDtypeStruct((2 * h0.shape[0], h0.shape[1]), h0.dtype),
        compiler_params=params(0),
        cost_estimate=cost(h0.size, 8 * h0.size),
        name="join",
    )(ids, h0, h1)


def weight_kernel(start, block, ids_ref, *refs):
    g0_ref, g1_ref, refs = refs[0], refs[1], refs[2:]
    h_ref, (o_ref, g_ref, r_ref, sem) = refs[0], refs[-4:]
    tokens, count = g0_ref.shape[0], g_ref.shape[1]
    mine = pl.multiple_of(ids_ref[1] * tokens, tokens)
    other = pl.multiple_of((1 - ids_ref[1]) * tokens, tokens)
    g_ref[pl.ds(mine, tokens), :] = g0_ref[:, start : start + count]
    g_ref[pl.ds(other, tokens), :] = g1_ref[:, start : start + count]
    turned = g_ref[...].T
    copies = []
    part = r_ref.shape[2]
    across = h_ref.shape[1] // part
    for i in range(r_ref.shape[0]):
        row, col = i // across * block, i % across * part
        r_ref[i] = jnp.dot(
            turned[row : row + block, :],
            h_ref[:, col : col + part],
            preferred_element_type=f32,
        )
        copies.append(
            pltpu.make_async_copy(
                r_ref.at[i],
                o_ref.at[pl.ds(start + row, block), pl.ds(col, part)],
                sem.at[i],
            )
        )
        copies[-1].start()
    for copy in copies:
        copy.wait()


def weight_call(ids, g0, g1, hs, start, count, block, into):
    tokens, rows = g0.shape
    width = hs[0].shape[1]
    hbm = pl.BlockSpec(memory_space=pltpu.HBM)
    first = into is None
    operands = [ids, g0, g1, *hs] + ([] if first else [into])
    specs = [smem()] + [vmem()] * (2 + len(hs)) + ([] if first else [hbm])
    across = 8
    steps = count // block * across
    return pl.pallas_call(
        functools.partial(weight_kernel, start, block),
        in_specs=specs,
        out_specs=hbm,
        out_shape=jax.ShapeDtypeStruct((rows, width), f32),
        scratch_shapes=[
            pltpu.VMEM((2 * tokens, count), bf16),
            pltpu.VMEM((steps, block, width // across), f32),
            pltpu.SemaphoreType.DMA((steps,)),
        ],
        input_output_aliases={} if first else {4: 0},
        compiler_params=params(0, 32),
        cost_estimate=cost(4 * tokens * count * width, 4 * count * width),
        name="weight",
    )(*operands)


def slide(x, by, n):
    half = n // 2
    return lax.ppermute(x, "seq", [(i, (i // 2 + by) % half * 2 + i % 2) for i in range(n)])


def swap(x, axis, mask, size):
    return lax.ppermute(x, axis, [(i, i ^ mask) for i in range(size)])


def split(total, unit):
    tiles = total // unit
    sizes = [tiles // 3, (tiles - tiles // 3 - 1) // 2, 0, 1]
    sizes[2] = tiles - sum(sizes)
    starts = [sum(sizes[:i]) for i in range(len(sizes))]
    return [(a * unit, c * unit) for a, c in zip(starts, sizes)]


def portions(total, unit):
    tiles = total // unit
    sizes = [tiles - tiles // 3 - 4, 3, tiles // 3, 1]
    starts = [sum(sizes[:i]) for i in range(len(sizes))]
    return [(a * unit, c * unit) for a, c in zip(starts, sizes)]


def sides(total, unit):
    tiles = total // unit
    sizes = [(tiles + 1) // 3, tiles // 4, tiles - (tiles + 1) // 3 - tiles // 4]
    starts = [sum(sizes[:i]) for i in range(len(sizes))]
    return [(a * unit, c * unit) for a, c in zip(starts, sizes)]


def fast(n, trunk, branch, unembed, targets, loss_grad):
    block_rows, width = unembed.shape
    seq_index = lax.axis_index("seq")
    ids = jnp.stack([seq_index, lax.axis_index("head"), seq_index * block_rows]).astype(jnp.int32)
    hidden = (trunk.astype(f32) + branch[0].astype(f32)).astype(bf16)
    far = [2 * (i + 1) for i in range(n // 2 - 1)]
    far = far[:1] + far[1:][::-1]

    pieces = [None] * n
    pieces[0] = hidden
    for k in far:
        pieces[k] = slide(hidden, -k // 2, n)
    for k in [0] + far:
        pieces[k + 1] = swap(pieces[k], "seq", 1, n)

    chunks = split(block_rows, 256)
    late = chunks[2][0]
    staged = [unembed]
    ids = tick_call(ids, 8 * unembed.size)
    places = tuple((0, start) for start, _ in chunks)

    def exchange(s):
        s = s.astype(f16)
        return s.astype(f32) + swap(s, "mp", 1, 2).astype(f32)

    late = [far[-1] + 1]
    soon = [k for k in range(n) if k not in late]
    order = (0, 1, 2, 3)
    scores = [None] * 4
    part = part_call([pieces[k] for k in soon], unembed, *chunks[0])
    most = exchange(part)
    for c in order[1:]:
        if c == 3:
            part = part_call([pieces[k] for k in late], unembed, *chunks[0])
            rest = exchange(part)
        if c == 1:
            s, all_hidden, turned = first_call(ids, pieces, unembed, *chunks[c])
        else:
            s = next_call(turned, unembed, *chunks[c])
        scores[c] = exchange(s)
    other_hidden = swap(all_hidden, "head", 1, 2)
    qs, ps, spread, so_far = [None] * 4, [None] * 4, None, None
    for c in (1, 2, 0, 3):
        first, last = c == 1, c == 3
        operands = [targets] if first else [spread, so_far]
        parts, groups = ([most, rest], (soon, late)) if c == 0 else ([scores[c]], None)
        qs[c], ps[c], *out = numer_call(
            chunks[c][0], first, last, n, groups, ids, parts, operands
        )
        if first:
            so_far, spread = out
        elif not last:
            so_far = out[0]
    total, stats = out
    sums = []
    for start, count in sides(width, 512):
        sums.append(rows_call(qs, staged, places, start, count, 512))
    for i in range(n.bit_length() - 1):
        total = total + swap(total, "seq", 1 << i, n)

    groups = ((4, 2), (6, 0))
    blocks = norm_call(n, groups, ids, total, stats, loss_grad, sums)
    keep, send = blocks[: n // 2], blocks[n // 2 :]
    rows = hidden.shape[0]
    got = []
    for i, group in enumerate(groups):
        theirs = swap(send[i], "seq", 1, n)
        for j, k in enumerate(group):
            both = keep[k // 2] + theirs[j * rows : (j + 1) * rows].astype(f32)
            if k:
                both = slide(both.astype(bf16), k // 2, n).astype(f32)
            got.append(both)
    row_grad = functools.reduce(lambda a, b: a + b, got)

    g = grads_call(ids, ps, spread, total, stats, loss_grad)
    g_other = swap(g, "head", 1, 2)
    hs = [join_call(ids, all_hidden, other_hidden)]
    d_unembed = None
    for start, count in portions(block_rows, 128):
        block = 128 if count % 256 else 256
        d_unembed = weight_call(ids, g, g_other, hs, start, count, block, d_unembed)

    d_trunk = row_grad + swap(row_grad, "head", 1, 2)
    return (row_grad.astype(bf16)[None], d_trunk.astype(bf16), d_unembed)


def general(trunk, branch, unembed, targets, loss_grad):
    block_rows = unembed.shape[0]
    hidden = (trunk.astype(f32) + branch[0].astype(f32)).astype(bf16)
    gathered = lax.all_gather(hidden, "seq", axis=0, tiled=True)
    seq_index = lax.axis_index("seq")
    scores = lax.psum(
        lax.dot_general(unembed, gathered, (((1,), (1,)), ((), ())), preferred_element_type=f32),
        "mp",
    )
    exponent, slope = soften(scores)
    totals = lax.psum(jnp.sum(exponent, axis=0), "seq")
    vocab_ids = seq_index * block_rows + lax.iota(jnp.int32, block_rows)
    onehot = (vocab_ids[:, None] == targets[0][None, :]).astype(f32)
    grad_logits = (
        loss_grad[0][None, :] * (exponent / totals[None, :] - onehot) * slope
    ).astype(bf16)
    row_grad = lax.psum_scatter(
        lax.dot_general(grad_logits, unembed, (((0,), (0,)), ((), ())), preferred_element_type=f32),
        "seq",
        scatter_dimension=0,
        tiled=True,
    )
    weight_grad = jnp.dot(grad_logits, gathered, preferred_element_type=f32)
    trunk_sum, unembed_sum = lax.psum((row_grad, weight_grad), "head")
    return (row_grad.astype(bf16)[None], trunk_sum.astype(bf16), unembed_sum)


def solution(mesh):
    in_specs = (
        P("seq", "mp"),
        P("head", "seq", "mp"),
        P("seq", "mp"),
        P("head", None),
        P("head", None),
    )
    out_specs = (P("head", "seq", "mp"), P("seq", "mp"), P("seq", "mp"))
    n = mesh.shape["seq"]
    if mesh.shape["head"] == 2 and mesh.shape["mp"] == 2 and n == 8:

        def body(*args):
            return fast(n, *args)
    else:
        body = general
    step = jax.shard_map(body, mesh=mesh, in_specs=in_specs, out_specs=out_specs, check_vma=False)
    if body is general:
        return step
    return step
```
